32 devices in a mesh: lat: 8 (over z, core), wave: 4 (over y, x).
Axes of the slice: x: 2, y: 2, z: 4, core: 2. Of those that a mesh axis runs over, the one named last changes fastest.
Arguments:
- spectra: bfloat16 [3, 2, 2, 768, 768], P(None, None, None, 'wave', 'lat'), may hold values from -0.01171875 to 0.01171875
- legendre: bfloat16 [16, 768, 768], P('lat', 'wave'), may hold values from -4 to 4
- wave_m: int32 [768], replicated, may hold values from 0 to 767, each once
- nlon: int32 [16], P('lat'), may hold values from 20 to 3088, as said below
- coriolis: float32 [16], P('lat'), may hold values from -1.5 to 1.5
- gauss_quadrature_weight: float32 [16], P('lat'), may hold values from 0.5 to 5
Outputs:
- tendency: float32 [2, 2, 2, 768, 768], P(None, None, None, 'wave', 'lat')
The draws below stay inside these ranges and needn't reach their ends.
Inputs may be any that keep to these rules, and one draw needn't show every extreme that they name: `nlon`: each value is 20 + 4 i for a whole number i, and some latitude has 3088. `wave_m`: every wavenumber 0 to 767 stands in exactly one slot.
All inputs are finite; a program needn't handle non-finite values.
Results may differ from the reference program's by a relative error of at most 0.0065.
Values may be sent and summed in bfloat16 or wider, within the bound.
No kernel may reach another device: no remote copies, remote signals or barrier semaphores. Data moves between devices by JAX's collectives and lax.ppermute only.
A program may use at most 64 MiB of HBM per device.

```python
import math
import jax
import jax.numpy as jnp
from jax import lax

WAVES = 768
NLON = 3088
LEV = 2
LAT_DEV = 2
LATS = 16
N_LAT = 8


def draw_nlon(key, part):
    first_key, second_key = jax.random.split(jax.random.fold_in(key, 11))
    indices = jax.random.randint(first_key, (LATS,), 0, WAVES)
    chosen = jax.random.randint(second_key, (), 0, LATS)
    indices = jnp.where(jnp.arange(LATS) == chosen, WAVES - 1, indices)
    return (20 + 4 * indices).astype(jnp.int32)


def shard_levels(own_key, extent, pieces, smallest, top_value):
    def one(axis_at, shards_of):
        steps = jax.random.uniform(jax.random.fold_in(jax.random.fold_in(own_key, 6), axis_at), (shards_of,), jnp.float32, smallest / len(pieces), top_value / len(pieces))
        return jnp.repeat(jnp.exp(steps), extent[axis_at] // shards_of).reshape((-1,) + (1,) * (len(extent) - axis_at - 1))

    gain = one(*pieces[0])
    for cut in pieces[1:]:
        gain = gain * one(*cut)
    return gain


def noise(own_key, extent, width, bound, shards=(), kind=jnp.bfloat16):
    level = shard_levels(own_key, extent, shards, -0.22, 0.18) if shards else 1.0
    array = jax.random.normal(own_key, extent, jnp.float32) * width * level
    return jnp.minimum(jnp.maximum(array, -bound), bound).astype(kind)


def setup_inputs(seed: int = 0) -> dict:
    seeds = jax.random.split(jax.random.key(seed), 7)
    return {
        "spectra": noise(seeds[0], (3, LEV, 2, WAVES, WAVES), (WAVES * WAVES // 2) ** -0.5, 0.01171875, ((3, 4), (4, 8))),
        "legendre": noise(seeds[1], (LATS, WAVES, WAVES), 1.0, 4.0, ((0, 8), (1, 4))),
        "wave_m": jax.random.permutation(seeds[2], WAVES).astype(jnp.int32),
        "nlon": draw_nlon(jax.random.fold_in(seeds[6], 71), 0),
        "coriolis": jnp.clip(jax.random.uniform(seeds[4], (LATS,), jnp.float32, -1.5, 1.5) * shard_levels(seeds[4], (LATS,), ((0, 8),), -0.4, 0.0), -1.5, 1.5),
        "gauss_quadrature_weight": jnp.clip(jnp.exp(math.log(5.0) - 2.3025851 * jax.random.uniform(seeds[5], (LATS,), jnp.float32) ** shard_levels(seeds[5], (LATS,), ((0, 8),), -0.2, 0.2)), 0.5, 5.0),
    }


lon_block = 512
two_pi = 6.283185307179586


def block_count():
    return (NLON + lon_block - 1) // lon_block


def column_factor(wave_ids, count):
    doubled = jnp.where(wave_ids == 0, jnp.float32(1.0), jnp.float32(2.0))
    return jnp.where(2 * wave_ids < count, doubled, jnp.float32(0.0))


def phase_table(wave_ids, first_place, count):
    places = first_place + jnp.arange(lon_block, dtype=jnp.int32)
    residue = (places[:, None] * wave_ids[None, :]) % count
    angles = (two_pi * residue.astype(jnp.float32)) / count.astype(jnp.float32)
    return jnp.concatenate([jnp.cos(angles), jnp.sin(angles)], axis=1).astype(jnp.bfloat16)


def inverse_stack(coefficient, multiplier):
    real_part = coefficient[..., 0, :].astype(jnp.float32) * multiplier
    imag_part = -coefficient[..., 1, :].astype(jnp.float32) * multiplier
    return jnp.concatenate([real_part, imag_part], axis=-1).astype(jnp.bfloat16)


def nonlinear(nodal_samples, rotation, places, count):
    vorticity = nodal_samples[..., 0, :]
    velocity_spread_map = nodal_samples[..., 1, :]
    thermal_state_map = nodal_samples[..., 2, :]
    stretch = -(vorticity + rotation) * velocity_spread_map
    thermal_forcing = -thermal_state_map * velocity_spread_map
    paired = jnp.stack([stretch, thermal_forcing], axis=-2)
    return jnp.where(places < count, paired, jnp.zeros_like(paired)).astype(jnp.bfloat16)


def finish(summed_spectra, multiplier, count, weight):
    halfway = summed_spectra.shape[-1] // 2
    scaling_factor = weight / count.astype(jnp.float32)
    real_part = summed_spectra[..., :halfway] * scaling_factor
    imag_part = -summed_spectra[..., halfway:] * scaling_factor
    paired = jnp.stack([real_part, imag_part], axis=-2)
    return jnp.where(multiplier > 0, paired, jnp.zeros_like(paired)).astype(jnp.bfloat16)


def grid_row(piled_arrays, wave_ids, count, rotation, weight, multiplier):
    def one_block(running, block_index):
        first_place = block_index * lon_block
        phases = phase_table(wave_ids, first_place, count)
        nodal_samples = lax.dot_general(piled_arrays, phases, (((1,), (1,)), ((), ())), preferred_element_type=jnp.float32)
        nodal_samples = nodal_samples.reshape(-1, 3, lon_block)
        places = first_place + jnp.arange(lon_block, dtype=jnp.int32)
        products = nonlinear(nodal_samples, rotation, places, count).reshape(-1, lon_block)
        return running + jnp.dot(products, phases, preferred_element_type=jnp.float32), None

    zero_sums = jnp.zeros((piled_arrays.shape[0] // 3 * 2, piled_arrays.shape[1]), jnp.float32)
    summed_spectra, unused = lax.scan(one_block, zero_sums, jnp.arange(block_count(), dtype=jnp.int32))
    return finish(summed_spectra.reshape(-1, 2, piled_arrays.shape[1]), multiplier, count, weight)


def reference(spectra, legendre, wave_m, nlon, coriolis, gauss_quadrature_weight):
    totals = jnp.arange(WAVES, dtype=jnp.int32)
    living = totals[None, :] >= wave_m[:, None]
    coeffs = spectra.astype(jnp.float32)

    def one_band(running, band_index):
        first_lat = (band_index * LAT_DEV).astype(jnp.int32)
        band_part = lax.dynamic_slice_in_dim(legendre, first_lat, LAT_DEV, 0)
        masked = jnp.where(living[None], band_part, jnp.zeros_like(band_part))
        widened = masked.astype(jnp.float32)
        fourier = jnp.einsum('lsn,fvpsn->lvfps', widened, coeffs).astype(jnp.bfloat16)
        counts = lax.dynamic_slice_in_dim(nlon, first_lat, LAT_DEV, 0)
        rotations = lax.dynamic_slice_in_dim(coriolis, first_lat, LAT_DEV, 0)
        weights = lax.dynamic_slice_in_dim(gauss_quadrature_weight, first_lat, LAT_DEV, 0)

        def latitude(inputs):
            coefficient, count, rotation, weight = inputs
            multiplier = column_factor(wave_m, count)
            piled_arrays = inverse_stack(coefficient.reshape(LEV * 3, 2, WAVES), multiplier)
            return grid_row(piled_arrays, wave_m, count, rotation, weight, multiplier)

        returned = lax.map(latitude, (fourier, counts, rotations, weights))
        partial_sums = jnp.einsum('lsn,lvqps->qvpsn', widened, returned.astype(jnp.float32))
        return running + partial_sums, None

    zero_sums = jnp.zeros((2, LEV, 2, WAVES, WAVES), jnp.float32)
    tendency, unused = lax.scan(one_band, zero_sums, jnp.arange(N_LAT, dtype=jnp.int32))
    return tendency
```

```python
import functools
import math

import jax
import jax.numpy as jnp
from jax import lax
from jax.experimental import pallas as pl
from jax.experimental.pallas import tpu as pltpu
from jax.sharding import PartitionSpec as P

NLON = 3088
BASE = 32

F32 = jnp.float32
BF16 = jnp.bfloat16


def whole(memory_space=pltpu.VMEM):
    return pl.BlockSpec(memory_space=memory_space)


def turn_kernel(ids_ref, legendre_ref, out_ref):
    total, columns = out_ref.shape
    ids = ids_ref[...]
    for first in range(0, total, 128):
        piece = legendre_ref[:, first : first + 128].astype(F32).T
        degrees = first + lax.broadcasted_iota(jnp.int32, piece.shape, 0)
        out_ref[first : first + 128, :] = jnp.where(degrees >= ids, piece, 0.0).astype(BF16)


def turn_spectra_kernel(repeats, spectra_ref, out_ref):
    slots = spectra_ref.shape[1]
    for i in range(spectra_ref.shape[0]):
        turned = spectra_ref[i].astype(F32).T
        out_ref[i] = jnp.concatenate([turned] * repeats, axis=1)


def forward_kernel(legendre_ref, spectra_ref, out_ref):
    sources, degrees, columns = legendre_ref.shape
    fields = spectra_ref.shape[0]

    def one_source(a, carry):
        piece = legendre_ref[a].astype(F32)
        rows = [
            jnp.sum(piece * spectra_ref[i], axis=0, keepdims=True) for i in range(fields)
        ]
        out_ref[a] = jnp.concatenate(rows, axis=0).astype(BF16)
        return carry

    lax.fori_loop(0, sources, one_source, 0)


def cos_sin(places, ids, count, inverse):
    quads = 4.0 * places * ids
    turns = jnp.floor(quads * inverse + 0.5)
    angle = (quads - turns * count) * (inverse * (math.pi / 2))
    square = angle * angle
    c = 1.0 + square * (-1 / 2 + square * (1 / 24 + square * (-1 / 720 + square * (1 / 40320))))
    s = angle * (
        1.0 + square * (-1 / 6 + square * (1 / 120 + square * (-1 / 5040 + square * (1 / 362880))))
    )
    quadrant = turns - 4.0 * jnp.floor(turns * 0.25)
    odd = (quadrant == 1.0) | (quadrant == 3.0)
    cosine = jnp.where(odd, s, c)
    sine = jnp.where(odd, c, s)
    cosine = jnp.where((quadrant == 1.0) | (quadrant == 2.0), -cosine, cosine)
    sine = jnp.where(quadrant >= 2.0, -sine, sine)
    return cosine, sine


def grid_kernel(
    lev_count, rank_ref, nlon_ref, coriolis_ref, weight_ref, fourier_ref, ids_ref, out_ref,
    base_ref, step_ref, table_ref, left_ref,
):
    owned, _, waves = fourier_ref.shape
    steps = step_ref.shape[1]
    places = BASE * steps
    ids = ids_ref[...].astype(F32)
    parity = 1.0 - 2.0 * (ids - 2.0 * jnp.floor(ids * 0.5))
    for offset in range(owned):
        latitude = (rank_ref[0] * owned + offset) // lev_count
        count_int = nlon_ref[latitude]
        count = jnp.full((1, waves), count_int.astype(F32))
        inverse = 1.0 / count
        rows = lax.broadcasted_iota(jnp.int32, (BASE, waves), 0).astype(F32)
        base_ref[0], base_ref[1] = cos_sin(rows, ids, count, inverse)
        rows = lax.broadcasted_iota(jnp.int32, (steps, waves), 0).astype(F32) * BASE
        step_ref[0], step_ref[1] = cos_sin(rows, ids, count, inverse)
        for a in range(steps):
            step_c = step_ref[0, a : a + 1, :]
            step_s = step_ref[1, a : a + 1, :]
            base_c = base_ref[0]
            base_s = base_ref[1]
            here = slice(a * BASE, (a + 1) * BASE)
            table_ref[here, :waves] = (step_c * base_c - step_s * base_s).astype(BF16)
            table_ref[here, waves:] = (step_s * base_c + step_c * base_s).astype(BF16)

        factor = jnp.where(ids == 0.0, 1.0, 2.0)
        factor = jnp.where(2.0 * ids < count, factor, 0.0)
        for field in range(3):
            real = fourier_ref[offset, 2 * field : 2 * field + 1, :].astype(F32) * factor
            imag = -fourier_ref[offset, 2 * field + 1 : 2 * field + 2, :].astype(F32) * factor
            first = jnp.concatenate([real, real, real * parity, real * parity], axis=0)
            second = jnp.concatenate([imag, -imag, -imag * parity, imag * parity], axis=0)
            pad = jnp.zeros((4, waves), F32)
            left_ref[8 * field : 8 * field + 8, :waves] = jnp.concatenate([first, pad], axis=0)
            left_ref[8 * field : 8 * field + 8, waves:] = jnp.concatenate([second, pad], axis=0)
        grid = lax.dot_general(
            left_ref[...].astype(BF16),
            table_ref[...],
            (((1,), (1,)), ((), ())),
            preferred_element_type=F32,
        )
        vorticity, divergence, temperature = grid[0:8], grid[8:16], grid[16:24]
        stretch = -(vorticity + coriolis_ref[latitude]) * divergence
        heating = -temperature * divergence
        quarter = count_int // 4
        place = lax.broadcasted_iota(jnp.int32, stretch.shape, 1)
        share = jnp.where((place == 0) | (place == quarter), 0.5, 1.0)

        def shared(product):
            rounded = jnp.where(place <= quarter, product, 0.0).astype(BF16)
            return rounded.astype(F32) * share

        products = jnp.concatenate([shared(stretch), shared(heating)], axis=0).astype(BF16)
        sums = jnp.dot(products, table_ref[...], preferred_element_type=F32)
        scale = weight_ref[latitude] / count
        for q in range(2):
            c = sums[8 * q : 8 * q + 4, :waves]
            s = sums[8 * q : 8 * q + 4, waves:]
            real = (c[0:1] + c[1:2]) + parity * (c[2:3] + c[3:4])
            imag = (s[0:1] - s[1:2]) + parity * (s[3:4] - s[2:3])
            both = jnp.concatenate([real * scale, -imag * scale], axis=0)
            both = jnp.where(factor > 0.0, both, 0.0).astype(BF16)
            out_ref[offset, 2 * q : 2 * q + 2, :] = both


def backward_kernel(lats, legendre_ref, back_ref, out_ref, turned_ref):
    sources, degrees, columns = legendre_ref.shape
    outs = back_ref.shape[1]
    slots = columns // lats
    for first in range(0, degrees, 8):
        last = min(first + 8, degrees)

        def one_source(a, sums):
            piece = legendre_ref[a, first:last, :].astype(F32)
            return tuple(
                total + piece * back_ref[a, i : i + 1, :] for i, total in enumerate(sums)
            )

        zero = jnp.zeros((last - first, columns), F32)
        sums = lax.fori_loop(0, sources, one_source, (zero,) * outs)
        for i in range(outs):
            folded = sums[i][:, :slots]
            for lat in range(1, lats):
                folded = folded + sums[i][:, lat * slots : (lat + 1) * slots]
            turned_ref[i, first:last, :] = folded
    for i in range(outs):
        out_ref[i] = turned_ref[i].T


def local(n_lat, n_wave, spectra, legendre, wave_m, nlon, coriolis, gauss_quadrature_weight):
    lats, slots, total = legendre.shape
    levels = spectra.shape[1]
    waves = wave_m.shape[0]
    degrees = spectra.shape[4]
    columns = lats * slots
    owned = lats * levels // n_wave
    wave_rank = lax.axis_index("wave")
    ids = lax.dynamic_slice_in_dim(wave_m, wave_rank * slots, slots, 0)
    ids = jnp.tile(ids, lats).reshape(1, columns)

    turned = pl.pallas_call(
        turn_kernel,
        out_shape=jax.ShapeDtypeStruct((total, columns), BF16),
        in_specs=[whole(), whole()],
        out_specs=whole(),
        name="turn",
    )(ids, legendre.reshape(columns, total))
    turned = lax.all_to_all(turned.reshape(n_lat, degrees, columns), "lat", 0, 0, tiled=True)

    spectra_turned = pl.pallas_call(
        functools.partial(turn_spectra_kernel, lats),
        out_shape=jax.ShapeDtypeStruct((6 * levels, degrees, columns), F32),
        in_specs=[whole()],
        out_specs=whole(),
        name="turn_spectra",
    )(spectra.reshape(6 * levels, slots, degrees))

    partial = pl.pallas_call(
        forward_kernel,
        out_shape=jax.ShapeDtypeStruct((n_lat, 6 * levels, columns), BF16),
        in_specs=[whole(), whole()],
        out_specs=whole(),
        name="forward",
    )(turned, spectra_turned)

    partial = partial.reshape(n_lat, 3, levels, 2, lats, slots).transpose(0, 4, 2, 1, 3, 5)
    partial = partial.reshape(n_lat * n_wave, owned, 6, slots)
    gathered = lax.all_to_all(partial, ("lat", "wave"), 0, 0, tiled=True)
    gathered = gathered.reshape(n_lat, n_wave, owned, 6, slots).astype(F32).sum(axis=0)
    fourier = gathered.transpose(1, 2, 0, 3).reshape(owned, 6, waves).astype(BF16)

    quarter_places = NLON // 4 + 1
    steps = -(-quarter_places // BASE)
    smem = whole(pltpu.SMEM)
    back = pl.pallas_call(
        functools.partial(grid_kernel, levels),
        out_shape=jax.ShapeDtypeStruct((owned, 4, waves), BF16),
        in_specs=[smem, smem, smem, smem, whole(), whole()],
        out_specs=whole(),
        scratch_shapes=[
            pltpu.VMEM((2, BASE, waves), F32),
            pltpu.VMEM((2, steps, waves), F32),
            pltpu.VMEM((steps * BASE, 2 * waves), BF16),
            pltpu.VMEM((24, 2 * waves), F32),
        ],
        name="grid",
    )(
        wave_rank.reshape(1),
        nlon,
        coriolis,
        gauss_quadrature_weight,
        fourier,
        wave_m.reshape(1, waves),
    )

    back = back.reshape(owned, 4, n_wave, slots).transpose(2, 0, 1, 3)
    back = jnp.broadcast_to(back[None], (n_lat,) + back.shape)
    back = back.reshape(n_lat * n_wave, owned, 4, slots)
    back = lax.all_to_all(back, ("lat", "wave"), 0, 0, tiled=True)
    back = back.reshape(n_lat, lats, levels, 2, 2, slots).transpose(0, 3, 2, 4, 1, 5)
    back = back.reshape(n_lat, 4 * levels, columns).astype(F32)

    out = pl.pallas_call(
        functools.partial(backward_kernel, lats),
        out_shape=jax.ShapeDtypeStruct((4 * levels, slots, degrees), F32),
        in_specs=[whole(), whole()],
        out_specs=whole(),
        scratch_shapes=[pltpu.VMEM((4 * levels, degrees, slots), F32)],
        name="backward",
    )(turned, back)
    return out.reshape(2, levels, 2, slots, degrees)


def solution(mesh):
    placed = (
        P(None, None, None, "wave", "lat"),
        P("lat", "wave", None),
        P(),
        P("lat"),
        P("lat"),
        P("lat"),
    )
    return jax.shard_map(
        functools.partial(local, mesh.shape["lat"], mesh.shape["wave"]),
        mesh=mesh,
        in_specs=placed,
        out_specs=P(None, None, None, "wave", "lat"),
        check_vma=False,
    )
```

```python
import functools
import math

import jax
import jax.numpy as jnp
from jax import lax
from jax.experimental import pallas as pl
from jax.experimental.pallas import tpu as pltpu
from jax.sharding import PartitionSpec as P

NLON = 3088
BASE = 32
LANES = 128

F32 = jnp.float32
BF16 = jnp.bfloat16

VMEM = pl.BlockSpec(memory_space=pltpu.VMEM)
SMEM = pl.BlockSpec(memory_space=pltpu.SMEM)
ANY = pl.BlockSpec(memory_space=pl.ANY)


def call(body, name, out_shape, in_specs, scratch=(), out_specs=VMEM, flops=0, bytes_accessed=0):
    return pl.pallas_call(
        body,
        out_shape=out_shape,
        in_specs=in_specs,
        out_specs=out_specs,
        scratch_shapes=scratch,
        name=name,
        cost_estimate=pl.CostEstimate(
            flops=flops, bytes_accessed=bytes_accessed, transcendentals=0
        ),
        compiler_params=pltpu.CompilerParams(vmem_limit_bytes=16 * 1024 * 1024),
    )


def pieces(extent, size):
    return [(first, min(first + size, extent)) for first in range(0, extent, size)]


def turn_kernel(legendre_ref, out_ref, held_ref, sems):
    parts = pieces(legendre_ref.shape[1], LANES)
    copies = []
    for i, (first, last) in enumerate(parts):
        copies.append(
            pltpu.make_async_copy(
                legendre_ref.at[:, first:last], held_ref.at[:, first:last], sems.at[i]
            )
        )
        copies[-1].start()
    for i, (first, last) in enumerate(parts):
        copies[i].wait()
        out_ref[first:last, :] = held_ref[:, first:last].T


def turn_spectra_kernel(repeats, fields, rank_ref, spectra_ref, ids_ref, out_ref):
    count, slots, degrees = spectra_ref.shape
    levels = count // (2 * fields)
    degree = rank_ref[0] * degrees + lax.broadcasted_iota(jnp.int32, (degrees, slots), 0)
    alive = degree >= ids_ref[...]
    for i in range(count):
        field, level, part = i // (2 * levels), (i // 2) % levels, i % 2
        turned = jnp.where(alive, spectra_ref[i].astype(F32).T, 0.0)
        place = (level * fields + field) * 2 + part
        out_ref[place] = jnp.concatenate([turned] * repeats, axis=1)


def forward_kernel(levels, owned, legendre_ref, spectra_ref, out_ref):
    sources, degrees, columns = legendre_ref.shape
    fields = spectra_ref.shape[0]
    per_level = fields // levels
    slots = out_ref.shape[-1]
    lats = columns // slots
    targets = out_ref.shape[0] // sources
    group = 2 if sources % 2 == 0 else 1

    def fold(value):
        total = value[0:8] if value.shape[0] >= 8 else value
        for first, last in pieces(value.shape[0], 8)[1:]:
            if last - first == 8:
                total = total + value[first:last]
        return total

    def some_sources(g, carry):
        tiles = [[] for _ in range(group)]
        for left, right in pieces(columns, LANES):
            sums = [[None] * fields for _ in range(group)]
            for first, last in pieces(degrees, 16):
                own = [
                    legendre_ref[g * group + k, first:last, left:right].astype(F32)
                    for k in range(group)
                ]
                for i in range(fields):
                    other = spectra_ref[i, first:last, left:right]
                    for k in range(group):
                        product = own[k] * other
                        rest = product.shape[0] % 8
                        if product.shape[0] > 8 and rest == 0:
                            product = fold(product)
                        else:
                            product = jnp.sum(product, axis=0, keepdims=True)
                        sums[k][i] = product if sums[k][i] is None else sums[k][i] + product
            for k in range(group):
                rows = [jnp.sum(value, axis=0, keepdims=True) for value in sums[k]]
                tiles[k].append(jnp.concatenate(rows, axis=0))
        for k in range(group):
            whole = jnp.concatenate(tiles[k], axis=1)
            for row in range(lats * levels):
                lat, level = row // levels, row % levels
                out_ref[(g * group + k) * targets + row // owned, row % owned] = whole[
                    level * per_level : (level + 1) * per_level,
                    lat * slots : (lat + 1) * slots,
                ].astype(BF16)
        return carry

    lax.fori_loop(0, sources // group, some_sources, 0)


def cos_sin(places, ids, count, inverse):
    quads = 4.0 * places * ids
    turns = jnp.floor(quads * inverse + 0.5)
    angle = (quads - turns * count) * (inverse * (math.pi / 2))
    square = angle * angle
    c = 1.0 + square * (-1 / 2 + square * (1 / 24 + square * (-1 / 720 + square * (1 / 40320))))
    s = angle * (
        1.0 + square * (-1 / 6 + square * (1 / 120 + square * (-1 / 5040 + square * (1 / 362880))))
    )
    quadrant = turns - 4.0 * jnp.floor(turns * 0.25)
    odd = (quadrant == 1.0) | (quadrant == 3.0)
    cosine = jnp.where(odd, s, c)
    sine = jnp.where(odd, c, s)
    cosine = jnp.where((quadrant == 1.0) | (quadrant == 2.0), -cosine, cosine)
    sine = jnp.where(quadrant >= 2.0, -sine, sine)
    return cosine, sine


def table_kernel(levels, rank_ref, nlon_ref, ids_ref, table_ref, base_ref, step_ref):
    owned = table_ref.shape[0]
    steps = step_ref.shape[1]
    waves = ids_ref.shape[1]
    ids = ids_ref[...].astype(F32)
    for offset in range(owned):
        latitude = (rank_ref[0] * owned + offset) // levels
        count = jnp.full((1, waves), nlon_ref[latitude].astype(F32))
        inverse = 1.0 / count
        rows = lax.broadcasted_iota(jnp.int32, (BASE, waves), 0).astype(F32)
        base_ref[0], base_ref[1] = cos_sin(rows, ids, count, inverse)
        rows = lax.broadcasted_iota(jnp.int32, (steps, waves), 0).astype(F32) * BASE
        step_ref[0], step_ref[1] = cos_sin(rows, ids, count, inverse)
        for a in range(steps):
            step_c = step_ref[0, a : a + 1, :]
            step_s = step_ref[1, a : a + 1, :]
            base_c = base_ref[0]
            base_s = base_ref[1]
            here = slice(a * BASE, (a + 1) * BASE)
            table_ref[offset, here, :waves] = (step_c * base_c - step_s * base_s).astype(BF16)
            table_ref[offset, here, waves:] = (step_s * base_c + step_c * base_s).astype(BF16)


def grid_kernel(
    levels, rank_ref, nlon_ref, coriolis_ref, weight_ref, partial_ref, table_ref, ids_ref, out_ref,
    left_ref,
):
    owned, _, slots = partial_ref.shape[1:]
    waves = ids_ref.shape[1]
    parts = waves // slots
    sources = partial_ref.shape[0] // parts
    ids = ids_ref[...].astype(F32)
    parity = 1.0 - 2.0 * (ids - 2.0 * jnp.floor(ids * 0.5))
    left_ref[...] = jnp.zeros_like(left_ref)
    for offset in range(owned):
        latitude = (rank_ref[0] * owned + offset) // levels
        count_int = nlon_ref[latitude]
        count = jnp.full((1, waves), count_int.astype(F32))

        def total(w):
            def add(a, value):
                return value + partial_ref[a * parts + w, offset].astype(F32)

            if sources > 8:
                return lax.fori_loop(1, sources, add, partial_ref[w, offset].astype(F32))
            value = partial_ref[w, offset].astype(F32)
            for a in range(1, sources):
                value = add(a, value)
            return value

        factor = jnp.where(ids == 0.0, 1.0, 2.0)
        factor = jnp.where(2.0 * ids < count, factor, 0.0)
        fourier = jnp.concatenate([total(w) for w in range(parts)], axis=1)
        fourier = fourier.astype(BF16).astype(F32) * factor
        for field in range(3):
            real = fourier[2 * field : 2 * field + 1]
            imag = -fourier[2 * field + 1 : 2 * field + 2]
            first = jnp.concatenate([real, real, real * parity, real * parity], axis=0)
            second = jnp.concatenate([imag, -imag, -imag * parity, imag * parity], axis=0)
            left_ref[8 * field : 8 * field + 4, :waves] = first
            left_ref[8 * field : 8 * field + 4, waves:] = second
        grid = lax.dot_general(
            left_ref[...].astype(BF16),
            table_ref[offset],
            (((1,), (1,)), ((), ())),
            preferred_element_type=F32,
        )
        vorticity, divergence, temperature = grid[0:8], grid[8:16], grid[16:24]
        stretch = -(vorticity + coriolis_ref[latitude]) * divergence
        heating = -temperature * divergence
        quarter = count_int // 4
        place = lax.broadcasted_iota(jnp.int32, stretch.shape, 1)
        share = jnp.where((place == 0) | (place == quarter), 0.5, 1.0)

        def shared(product):
            rounded = jnp.where(place <= quarter, product, 0.0).astype(BF16)
            return rounded.astype(F32) * share

        products = jnp.concatenate([shared(stretch), shared(heating)], axis=0).astype(BF16)
        sums = jnp.dot(products, table_ref[offset], preferred_element_type=F32)
        scale = weight_ref[latitude] / count
        both = []
        for q in range(2):
            c = sums[8 * q : 8 * q + 4, :waves]
            s = sums[8 * q : 8 * q + 4, waves:]
            real = (c[0:1] + c[1:2]) + parity * (c[2:3] + c[3:4])
            imag = (s[0:1] - s[1:2]) + parity * (s[3:4] - s[2:3])
            both += [real * scale, -imag * scale]
        back = jnp.concatenate(both, axis=0)
        back = jnp.where(factor > 0.0, back, 0.0).astype(BF16)
        for w in range(parts):
            part = back[:, w * slots : (w + 1) * slots]

            def put(a, carry):
                out_ref[a * parts + w, offset] = part
                return carry

            if sources > 8:
                lax.fori_loop(0, sources, put, 0)
            else:
                for a in range(sources):
                    put(a, 0)


def backward_kernel(
    levels, rank_ref, legendre_ref, back_ref, ids_ref, out_ref, wide_ref, sums_ref, done_ref, sems
):
    sources, degrees, columns = legendre_ref.shape
    outs, slots, _ = out_ref.shape
    lats = columns // slots
    owned = back_ref.shape[1]
    targets = back_ref.shape[0] // sources
    group = min(sources, 8)

    def spread(a, carry):
        for level in range(levels):
            rows = []
            for lat in range(lats):
                row = lat * levels + level
                rows.append(back_ref[a * targets + row // owned, row % owned].astype(F32))
            both = jnp.concatenate(rows, axis=1)
            for i in range(4):
                place = ((i // 2) * levels + level) * 2 + i % 2
                wide_ref[a, place] = jnp.broadcast_to(both[i : i + 1], (8, columns))
        return carry

    if sources > 8:
        lax.fori_loop(0, sources, spread, 0)
    else:
        for a in range(sources):
            spread(a, 0)

    for first, last in pieces(degrees, 16):
        for left, right in pieces(columns, LANES):

            def some_sources(g, sums):
                sums = list(sums)
                for k in range(group):
                    piece = legendre_ref[g * group + k, first:last, left:right].astype(F32)
                    for i in range(outs):
                        other = wide_ref[g * group + k, i, :, left:right]
                        other = jnp.concatenate([other, other], axis=0)[: last - first]
                        sums[i] = sums[i] + piece * other
                return tuple(sums)

            sums = (jnp.zeros((last - first, right - left), F32),) * outs
            if sources == group:
                sums = some_sources(0, sums)
            else:
                sums = lax.fori_loop(0, sources // group, some_sources, sums)
            for i in range(outs):
                sums_ref[i, first:last, left:right] = sums[i]

    degree = rank_ref[0] * degrees + lax.broadcasted_iota(jnp.int32, (degrees, slots), 0)
    alive = degree >= ids_ref[...]
    copies = []
    for i in range(outs):
        value = sums_ref[i]
        folded = value[:, :slots]
        for lat in range(1, lats):
            folded = folded + value[:, lat * slots : (lat + 1) * slots]
        done_ref[i] = jnp.where(alive, folded, 0.0).T
        copies.append(pltpu.make_async_copy(done_ref.at[i], out_ref.at[i], sems.at[i]))
        copies[-1].start()
    for copy in copies:
        copy.wait()


def local(n_lat, n_wave, spectra, legendre, wave_m, nlon, coriolis, gauss_quadrature_weight):
    lats, slots, total = legendre.shape
    fields, levels = spectra.shape[:2]
    waves = wave_m.shape[0]
    degrees = spectra.shape[4]
    columns = lats * slots
    owned = lats * levels // n_wave
    lat_rank = lax.axis_index("lat").reshape(1)
    wave_rank = lax.axis_index("wave").reshape(1)
    steps = -(-(NLON // 4 + 1) // BASE)

    turned = call(
        turn_kernel,
        "turn",
        jax.ShapeDtypeStruct((total, columns), BF16),
        [ANY],
        [pltpu.VMEM((columns, total), BF16), pltpu.SemaphoreType.DMA((-(-total // LANES),))],
        bytes_accessed=4 * total * columns,
    )(legendre.reshape(columns, total))
    turned = lax.all_to_all(turned.reshape(n_lat, degrees, columns), "lat", 0, 0, tiled=True)

    own_ids = lax.dynamic_slice_in_dim(wave_m, wave_rank[0] * slots, slots, 0).reshape(1, slots)
    all_ids = wave_m.reshape(1, waves)
    spectra_turned = call(
        functools.partial(turn_spectra_kernel, lats, fields),
        "turn_spectra",
        jax.ShapeDtypeStruct((2 * fields * levels, degrees, columns), F32),
        [SMEM, VMEM, VMEM],
        flops=10 * fields * levels * degrees * columns,
        bytes_accessed=8 * fields * levels * degrees * columns,
    )(lat_rank, spectra.reshape(2 * fields * levels, slots, degrees), own_ids)

    table = call(
        functools.partial(table_kernel, levels),
        "table",
        jax.ShapeDtypeStruct((owned, steps * BASE, 2 * waves), BF16),
        [SMEM, SMEM, VMEM],
        [pltpu.VMEM((2, BASE, waves), F32), pltpu.VMEM((2, steps, waves), F32)],
        flops=16 * owned * steps * BASE * waves,
        bytes_accessed=4 * owned * steps * BASE * waves,
    )(wave_rank, nlon, all_ids)

    partial = call(
        functools.partial(forward_kernel, levels, owned),
        "forward",
        jax.ShapeDtypeStruct((n_lat * n_wave, owned, 2 * fields, slots), BF16),
        [VMEM, VMEM],
        flops=4 * n_lat * fields * levels * degrees * columns,
        bytes_accessed=8 * fields * levels * degrees * columns,
    )(turned, spectra_turned)
    partial = lax.all_to_all(partial, ("lat", "wave"), 0, 0, tiled=True)

    back = call(
        functools.partial(grid_kernel, levels),
        "grid",
        jax.ShapeDtypeStruct((n_lat * n_wave, owned, 4, slots), BF16),
        [SMEM, SMEM, SMEM, SMEM, VMEM, VMEM, VMEM],
        [pltpu.VMEM((24, 2 * waves), F32)],
        flops=128 * owned * steps * BASE * waves,
        bytes_accessed=4 * owned * steps * BASE * waves,
    )(wave_rank, nlon, coriolis, gauss_quadrature_weight, partial, table, all_ids)
    back = lax.all_to_all(back, ("lat", "wave"), 0, 0, tiled=True)

    outs = 4 * levels
    out = call(
        functools.partial(backward_kernel, levels),
        "backward",
        jax.ShapeDtypeStruct((outs, slots, degrees), F32),
        [SMEM, VMEM, VMEM, VMEM],
        [
            pltpu.VMEM((n_lat, outs, 8, columns), F32),
            pltpu.VMEM((outs, degrees, columns), F32),
            pltpu.VMEM((outs, slots, degrees), F32),
            pltpu.SemaphoreType.DMA((outs,)),
        ],
        out_specs=ANY,
        flops=2 * n_lat * outs * degrees * columns,
        bytes_accessed=8 * outs * degrees * slots,
    )(lat_rank, turned, back, own_ids)
    return out.reshape(2, levels, 2, slots, degrees)


def solution(mesh):
    placed = (
        P(None, None, None, "wave", "lat"),
        P("lat", "wave", None),
        P(),
        P("lat"),
        P("lat"),
        P("lat"),
    )
    return jax.shard_map(
        functools.partial(local, mesh.shape["lat"], mesh.shape["wave"]),
        mesh=mesh,
        in_specs=placed,
        out_specs=P(None, None, None, "wave", "lat"),
        check_vma=False,
    )
```

```python
import functools
import math

import jax
import jax.numpy as jnp
from jax import lax
from jax.experimental import pallas as pl
from jax.experimental.pallas import tpu as pltpu
from jax.sharding import PartitionSpec as P

NLON = 3088
BASE = 16
LANES = 128

F32 = jnp.float32
BF16 = jnp.bfloat16

VMEM = pl.BlockSpec(memory_space=pltpu.VMEM)
SMEM = pl.BlockSpec(memory_space=pltpu.SMEM)
HBM = pl.BlockSpec(memory_space=pltpu.HBM)


def call(
    body, name, out_shape, in_specs, scratch=(), out_specs=VMEM, flops=0, bytes_accessed=0,
    grant=16 * 1024 * 1024,
):
    return pl.pallas_call(
        body,
        out_shape=out_shape,
        in_specs=in_specs,
        out_specs=out_specs,
        scratch_shapes=scratch,
        name=name,
        cost_estimate=pl.CostEstimate(
            flops=flops, bytes_accessed=bytes_accessed, transcendentals=0
        ),
        compiler_params=pltpu.CompilerParams(vmem_limit_bytes=grant),
    )


def pieces(extent, size):
    return [(first, min(first + size, extent)) for first in range(0, extent, size)]


def message_shape(rows, slots):
    if slots > LANES and slots % LANES == LANES // 2 and rows % 2 == 0:
        lines = rows * (slots // LANES) + rows // 2
        return (-(-lines // 2), 2, LANES)
    return (rows, slots)


def put_message(ref, index, value):
    if len(ref.shape) == len(index) + 2:
        ref[index] = value.astype(BF16)
        return
    rows, slots = value.shape
    lines = [value[:, first : first + LANES] for first in range(0, slots - LANES + 1, LANES)]
    rest = value[:, slots - LANES // 2 :]
    lines.append(jnp.concatenate([rest[: rows // 2], rest[rows // 2 :]], axis=1))
    if lines[-1].shape[0] % 2:
        lines.append(lines[-1][:1])
    lines = jnp.concatenate(lines, axis=0)
    for k in range(lines.shape[0] // 2):
        ref[index + (k,)] = lines[2 * k : 2 * k + 2].astype(BF16)


def get_message(message, rows, slots):
    if message.ndim == 2:
        return message
    lines = jnp.concatenate([message[k] for k in range(message.shape[0])], axis=0)
    whole = slots // LANES
    parts = [lines[k * rows : (k + 1) * rows] for k in range(whole)]
    rest = lines[whole * rows : whole * rows + rows // 2]
    half = LANES // 2
    parts.append(jnp.concatenate([rest[:, :half], rest[:, half:]], axis=0))
    return jnp.concatenate(parts, axis=1)


def turn_kernel(begin, legendre_ref, out_ref, held_ref, turned_ref, sems):
    width = out_ref.shape[1]
    parts = pieces(legendre_ref.shape[1], 2 * LANES)
    arrivals, departures = [], []
    for i, (first, last) in enumerate(parts):
        arrivals.append(
            pltpu.make_async_copy(
                legendre_ref.at[begin : begin + width, first:last],
                held_ref.at[:, first:last],
                sems.at[0, i],
            )
        )
        arrivals[-1].start()
    for i, (first, last) in enumerate(parts):
        arrivals[i].wait()
        turned_ref[first:last, :] = held_ref[:, first:last].T
        departures.append(
            pltpu.make_async_copy(turned_ref.at[first:last], out_ref.at[first:last], sems.at[1, i])
        )
        departures[-1].start()
    for copy in departures:
        copy.wait()


def turn_spectra_kernel(repeats, fields, rank_ref, spectra_ref, ids_ref, out_ref):
    count, slots, degrees = spectra_ref.shape
    levels = count // (2 * fields)
    degree = rank_ref[0] * degrees + lax.broadcasted_iota(jnp.int32, (degrees, slots), 0)
    alive = degree >= ids_ref[...]
    for i in range(count):
        field, level, part = i // (2 * levels), (i // 2) % levels, i % 2
        turned = jnp.where(alive, spectra_ref[i].astype(F32).T, 0.0)
        place = (level * fields + field) * 2 + part
        out_ref[place] = jnp.concatenate([turned] * repeats, axis=1)


def forward_sums(begin, g, group, legendre_ref, spectra_ref):
    degrees, width = legendre_ref.shape[1:]
    fields = spectra_ref.shape[0]
    tiles = [[] for _ in range(group)]
    for left, right in pieces(width, LANES):
        sums = [[None] * fields for _ in range(group)]
        for first, last in pieces(degrees, 16):
            own = [
                legendre_ref[g * group + k, first:last, left:right].astype(F32)
                for k in range(group)
            ]
            for i in range(fields):
                other = spectra_ref[i, first:last, begin + left : begin + right]
                for k in range(group):
                    product = own[k] * other
                    if last - first == 16:
                        product = product[:8] + product[8:]
                    else:
                        product = jnp.sum(product, axis=0, keepdims=True)
                    sums[k][i] = product if sums[k][i] is None else sums[k][i] + product
        for k in range(group):
            rows = [jnp.sum(value, axis=0, keepdims=True) for value in sums[k]]
            tiles[k].append(jnp.concatenate(rows, axis=0))
    return [jnp.concatenate(tile, axis=1) for tile in tiles]


def early_forward_kernel(begin, legendre_ref, spectra_ref, out_ref):
    sources = legendre_ref.shape[0]
    group = 2 if sources % 2 == 0 else 1

    def some_sources(g, carry):
        for k, value in enumerate(forward_sums(begin, g, group, legendre_ref, spectra_ref)):
            out_ref[g * group + k] = value
        return carry

    lax.fori_loop(0, sources // group, some_sources, 0)


def last_forward_kernel(begin, levels, owned, slots, legendre_ref, spectra_ref, *refs):
    *early_refs, out_ref = refs
    sources = legendre_ref.shape[0]
    fields = spectra_ref.shape[0]
    columns = spectra_ref.shape[2]
    per_level = fields // levels
    lats = columns // slots
    targets = out_ref.shape[0] // sources
    group = 2 if sources % 2 == 0 else 1

    def some_sources(g, carry):
        for k, value in enumerate(forward_sums(begin, g, group, legendre_ref, spectra_ref)):
            a = g * group + k
            value = jnp.concatenate([ref[a] for ref in early_refs] + [value], axis=1)
            for row in range(lats * levels):
                lat, level = row // levels, row % levels
                message = value[
                    level * per_level : (level + 1) * per_level,
                    lat * slots : (lat + 1) * slots,
                ]
                put_message(out_ref, (a * targets + row // owned, row % owned), message)
        return carry

    lax.fori_loop(0, sources // group, some_sources, 0)


def cos_sin(places, ids, count, inverse):
    quads = 4.0 * places * ids
    turns = jnp.floor(quads * inverse + 0.5)
    angle = (quads - turns * count) * (inverse * (math.pi / 2))
    square = angle * angle
    c = 1.0 + square * (-1 / 2 + square * (1 / 24 + square * (-1 / 720 + square * (1 / 40320))))
    s = angle * (
        1.0 + square * (-1 / 6 + square * (1 / 120 + square * (-1 / 5040 + square * (1 / 362880))))
    )
    quadrant = turns - 4.0 * jnp.floor(turns * 0.25)
    odd = (quadrant == 1.0) | (quadrant == 3.0)
    cosine = jnp.where(odd, s, c)
    sine = jnp.where(odd, c, s)
    cosine = jnp.where((quadrant == 1.0) | (quadrant == 2.0), -cosine, cosine)
    sine = jnp.where(quadrant >= 2.0, -sine, sine)
    return cosine, sine


def image_signs(ids):
    quadrant = ids - 4.0 * jnp.floor(ids * 0.25)
    one = jnp.ones_like(ids)
    none = jnp.zeros_like(ids)
    parity = jnp.where((quadrant == 1.0) | (quadrant == 3.0), -1.0, 1.0)
    c = jnp.where(quadrant == 0.0, 1.0, jnp.where(quadrant == 2.0, -1.0, 0.0))
    s = jnp.where(quadrant == 1.0, 1.0, jnp.where(quadrant == 3.0, -1.0, 0.0))
    cos_cos = [one, one, parity, parity, c, c, c, c]
    cos_sin = [none, none, none, none, s, -s, -s, s]
    sin_cos = [none, none, none, none, s, s, -s, -s]
    sin_sin = [one, -one, -parity, parity, -c, c, -c, c]
    return [jnp.concatenate(rows, axis=0) for rows in (cos_cos, cos_sin, sin_cos, sin_sin)]


def table_kernel(
    levels, rank_ref, nlon_ref, coriolis_ref, weight_ref, ids_ref,
    table_ref, left_ref, right_ref, share_ref, rotation_ref, base_ref, step_ref,
):
    owned = table_ref.shape[0]
    steps = step_ref.shape[1]
    waves = ids_ref.shape[1]
    ids = ids_ref[...].astype(F32)
    signs = image_signs(ids)
    for offset in range(owned):
        latitude = (rank_ref[0] * owned + offset) // levels
        count_int = nlon_ref[latitude]
        count = jnp.full((1, waves), count_int.astype(F32))
        inverse = 1.0 / count
        rows = lax.broadcasted_iota(jnp.int32, (BASE, waves), 0).astype(F32)
        base_ref[0], base_ref[1] = cos_sin(rows, ids, count, inverse)
        rows = lax.broadcasted_iota(jnp.int32, (steps, waves), 0).astype(F32) * BASE
        step_ref[0], step_ref[1] = cos_sin(rows, ids, count, inverse)
        for a in range(steps):
            step_c = step_ref[0, a : a + 1, :]
            step_s = step_ref[1, a : a + 1, :]
            base_c = base_ref[0]
            base_s = base_ref[1]
            here = slice(a * BASE, (a + 1) * BASE)
            table_ref[offset, here, :waves] = (step_c * base_c - step_s * base_s).astype(BF16)
            table_ref[offset, here, waves:] = (step_s * base_c + step_c * base_s).astype(BF16)

        factor = jnp.where(ids == 0.0, 1.0, 2.0)
        factor = jnp.where(2.0 * ids < count, factor, 0.0)
        scale = jnp.where(factor > 0.0, weight_ref[latitude] / count, 0.0)
        left_ref[offset, 0] = signs[0] * factor
        left_ref[offset, 1] = -signs[2] * factor
        left_ref[offset, 2] = signs[1] * factor
        left_ref[offset, 3] = -signs[3] * factor
        right_ref[offset, 0] = signs[0] * scale
        right_ref[offset, 1] = signs[1] * scale
        right_ref[offset, 2] = -signs[2] * scale
        right_ref[offset, 3] = -signs[3] * scale
        place = lax.broadcasted_iota(jnp.int32, share_ref.shape[1:], 1)
        share = jnp.where((place == 0) | (8 * place == count_int), 0.5, 1.0)
        share_ref[offset] = jnp.where(8 * place <= count_int, share, 0.0)
        rotation_ref[offset] = jnp.full(rotation_ref.shape[1:], coriolis_ref[latitude])


def grid_kernel(
    slots, partial_ref, table_ref, left_ref, right_ref, share_ref, rotation_ref, out_ref, rows_ref
):
    owned = partial_ref.shape[1]
    waves = left_ref.shape[-1]
    parts = waves // slots
    sources = partial_ref.shape[0] // parts
    for offset in range(owned):

        def total(w):
            def add(a, value):
                return value + partial_ref[a * parts + w, offset].astype(F32)

            if sources > 8:
                return lax.fori_loop(1, sources, add, partial_ref[w, offset].astype(F32))
            value = partial_ref[w, offset].astype(F32)
            for a in range(1, sources):
                value = add(a, value)
            return value

        fourier = jnp.concatenate(
            [get_message(total(w), 6, slots) for w in range(parts)], axis=1
        )
        fourier = fourier.astype(BF16).astype(F32)
        for field in range(3):
            here = slice(8 * field, 8 * field + 8)
            real = fourier[2 * field : 2 * field + 1]
            imag = fourier[2 * field + 1 : 2 * field + 2]
            rows_ref[here, :waves] = real * left_ref[offset, 0] + imag * left_ref[offset, 1]
            rows_ref[here, waves:] = real * left_ref[offset, 2] + imag * left_ref[offset, 3]
        grid = lax.dot_general(
            rows_ref[...].astype(BF16),
            table_ref[offset],
            (((1,), (1,)), ((), ())),
            preferred_element_type=F32,
        )
        vorticity, divergence, temperature = grid[0:8], grid[8:16], grid[16:24]
        share = share_ref[offset]

        def shared(product):
            rounded = jnp.where(share > 0.0, product, 0.0).astype(BF16)
            return rounded.astype(F32) * share

        stretch = shared(-(vorticity + rotation_ref[offset]) * divergence)
        heating = shared(-temperature * divergence)
        products = jnp.concatenate([stretch, heating], axis=0).astype(BF16)
        sums = jnp.dot(products, table_ref[offset], preferred_element_type=F32)
        both = []
        for q in range(2):
            c = sums[8 * q : 8 * q + 8, :waves]
            s = sums[8 * q : 8 * q + 8, waves:]
            for k in range(2):
                term = c * right_ref[offset, 2 * k] + s * right_ref[offset, 2 * k + 1]
                both.append(jnp.sum(term, axis=0, keepdims=True))
        back = jnp.concatenate(both, axis=0)
        for w in range(parts):
            part = back[:, w * slots : (w + 1) * slots]

            def put(a, carry):
                put_message(out_ref, (a * parts + w, offset), part)
                return carry

            if sources > 8:
                lax.fori_loop(0, sources, put, 0)
            else:
                for a in range(sources):
                    put(a, 0)


def backward_kernel(
    levels, rank_ref, back_ref, ids_ref, *refs
):
    *legendre_refs, out_ref, wide_ref, sums_ref, done_ref, sems = refs
    sources, degrees = legendre_refs[0].shape[:2]
    columns = wide_ref.shape[3]
    outs, slots, _ = out_ref.shape
    lats = columns // slots
    owned = back_ref.shape[1]
    targets = back_ref.shape[0] // sources
    group = min(sources, 8)

    def spread(a, carry):
        for level in range(levels):
            rows = []
            for lat in range(lats):
                row = lat * levels + level
                message = back_ref[a * targets + row // owned, row % owned].astype(F32)
                rows.append(get_message(message, 4, slots))
            both = jnp.concatenate(rows, axis=1)
            for i in range(4):
                place = ((i // 2) * levels + level) * 2 + i % 2
                wide_ref[a, place] = jnp.broadcast_to(both[i : i + 1], (8, columns))
        return carry

    if sources > 8:
        lax.fori_loop(0, sources, spread, 0)
    else:
        for a in range(sources):
            spread(a, 0)

    degree = rank_ref[0] * degrees + lax.broadcasted_iota(jnp.int32, (degrees, slots), 0)
    alive = degree >= ids_ref[...]
    tiles = []
    begin = 0
    for legendre_ref in legendre_refs:
        width = legendre_ref.shape[2]
        tiles += [(legendre_ref, begin, *piece) for piece in pieces(width, LANES)]
        begin += width
    copies = []
    for own in pieces(outs, 4):
        for first, last in pieces(degrees, 16):
            for legendre_ref, begin, left, right in tiles:
                whole = slice(begin + left, begin + right)

                def some_sources(g, sums):
                    sums = list(sums)
                    for k in range(group):
                        piece = legendre_ref[g * group + k, first:last, left:right].astype(F32)
                        for i in range(*own):
                            other = wide_ref[g * group + k, i, :, whole]
                            other = jnp.concatenate([other, other], axis=0)[: last - first]
                            term = piece * other
                            past = sums[i - own[0]]
                            sums[i - own[0]] = term if past is None else past + term
                    return tuple(sums)

                if sources == group:
                    sums = some_sources(0, (None,) * (own[1] - own[0]))
                else:
                    zero = jnp.zeros((last - first, right - left), F32)
                    sums = (zero,) * (own[1] - own[0])
                    sums = lax.fori_loop(0, sources // group, some_sources, sums)
                for i in range(*own):
                    sums_ref[i, first:last, whole] = sums[i - own[0]]
        for i in range(*own):
            value = sums_ref[i]
            folded = value[:, :slots]
            for lat in range(1, lats):
                folded = folded + value[:, lat * slots : (lat + 1) * slots]
            done_ref[i] = jnp.where(alive, folded, 0.0).T
            copies.append(pltpu.make_async_copy(done_ref.at[i], out_ref.at[i], sems.at[i]))
            copies[-1].start()
    for copy in copies:
        copy.wait()


def local(n_lat, n_wave, spectra, legendre, wave_m, nlon, coriolis, gauss_quadrature_weight):
    lats, slots, total = legendre.shape
    fields, levels = spectra.shape[:2]
    waves = wave_m.shape[0]
    degrees = spectra.shape[4]
    columns = lats * slots
    owned = lats * levels // n_wave
    lat_rank = lax.axis_index("lat").reshape(1)
    wave_rank = lax.axis_index("wave").reshape(1)
    steps = -(-(NLON // 8 + 1) // BASE)
    places = steps * BASE

    chunks = [(0, columns)]
    turned = []
    for begin, end in chunks:
        width = end - begin
        chunk = call(
            functools.partial(turn_kernel, begin),
            "turn",
            jax.ShapeDtypeStruct((total, width), BF16),
            [HBM],
            [
                pltpu.VMEM((width, total), BF16),
                pltpu.VMEM((total, width), BF16),
                pltpu.SemaphoreType.DMA((2, -(-total // (2 * LANES)))),
            ],
            out_specs=HBM,
            bytes_accessed=4 * total * width,
            grant=None,
        )(legendre.reshape(columns, total))
        chunk = chunk.reshape(n_lat, degrees, width)
        turned.append(lax.all_to_all(chunk, "lat", 0, 0, tiled=True))

    own_ids = lax.dynamic_slice_in_dim(wave_m, wave_rank[0] * slots, slots, 0).reshape(1, slots)
    all_ids = wave_m.reshape(1, waves)
    spectra_turned = call(
        functools.partial(turn_spectra_kernel, lats, fields),
        "turn_spectra",
        jax.ShapeDtypeStruct((2 * fields * levels, degrees, columns), F32),
        [SMEM, VMEM, VMEM],
        flops=10 * fields * levels * degrees * columns,
        bytes_accessed=8 * fields * levels * degrees * columns,
    )(lat_rank, spectra.reshape(2 * fields * levels, slots, degrees), own_ids)

    row = call(
        functools.partial(table_kernel, levels),
        "table",
        (
            jax.ShapeDtypeStruct((owned, places, 2 * waves), BF16),
            jax.ShapeDtypeStruct((owned, 4, 8, waves), F32),
            jax.ShapeDtypeStruct((owned, 4, 8, waves), F32),
            jax.ShapeDtypeStruct((owned, 8, places), F32),
            jax.ShapeDtypeStruct((owned, 8, places), F32),
        ),
        [SMEM, SMEM, SMEM, SMEM, VMEM],
        [pltpu.VMEM((2, BASE, waves), F32), pltpu.VMEM((2, steps, waves), F32)],
        out_specs=(VMEM,) * 5,
        flops=16 * owned * places * waves,
        bytes_accessed=4 * owned * places * waves,
    )(wave_rank, nlon, coriolis, gauss_quadrature_weight, all_ids)
    spectra_turned, *row = lax.optimization_barrier((spectra_turned, *row))

    early = []
    for (begin, end), chunk in zip(chunks[:-1], turned[:-1]):
        early.append(
            call(
                functools.partial(early_forward_kernel, begin),
                "early_forward",
                jax.ShapeDtypeStruct((n_lat, 2 * fields * levels, end - begin), F32),
                [VMEM, VMEM],
                flops=4 * n_lat * fields * levels * degrees * (end - begin),
                bytes_accessed=8 * fields * levels * degrees * (end - begin),
            )(chunk, spectra_turned)
        )
    begin, end = chunks[-1]
    partial = call(
        functools.partial(last_forward_kernel, begin, levels, owned, slots),
        "forward",
        jax.ShapeDtypeStruct((n_lat * n_wave, owned) + message_shape(2 * fields, slots), BF16),
        [VMEM, VMEM] + [VMEM] * len(early),
        flops=4 * n_lat * fields * levels * degrees * (end - begin),
        bytes_accessed=8 * fields * levels * degrees * (end - begin),
    )(turned[-1], spectra_turned, *early)
    partial = lax.all_to_all(partial, ("lat", "wave"), 0, 0, tiled=True)

    back = call(
        functools.partial(grid_kernel, slots),
        "grid",
        jax.ShapeDtypeStruct((n_lat * n_wave, owned, 4, slots), BF16),
        [VMEM] * 6,
        [pltpu.VMEM((24, 2 * waves), F32)],
        flops=128 * owned * places * waves,
        bytes_accessed=4 * owned * places * waves,
    )(partial, *row)
    back = lax.all_to_all(back, ("lat", "wave"), 0, 0, tiled=True)

    outs = 4 * levels
    out = call(
        functools.partial(backward_kernel, levels),
        "backward",
        jax.ShapeDtypeStruct((outs, slots, degrees), F32),
        [SMEM, VMEM, VMEM] + [VMEM] * len(turned),
        [
            pltpu.VMEM((n_lat, outs, 8, columns), F32),
            pltpu.VMEM((outs, degrees, columns), F32),
            pltpu.VMEM((outs, slots, degrees), F32),
            pltpu.SemaphoreType.DMA((outs,)),
        ],
        out_specs=HBM,
        flops=2 * n_lat * outs * degrees * columns,
        bytes_accessed=8 * outs * degrees * slots,
    )(lat_rank, back, own_ids, *turned)
    return out.reshape(2, levels, 2, slots, degrees)


def solution(mesh):
    placed = (
        P(None, None, None, "wave", "lat"),
        P("lat", "wave", None),
        P(),
        P("lat"),
        P("lat"),
        P("lat"),
    )
    return jax.shard_map(
        functools.partial(local, mesh.shape["lat"], mesh.shape["wave"]),
        mesh=mesh,
        in_specs=placed,
        out_specs=P(None, None, None, "wave", "lat"),
        check_vma=False,
    )
```

```python
import functools
import math

import jax
import jax.numpy as jnp
from jax import lax
from jax.experimental import pallas as pl
from jax.experimental.pallas import tpu as pltpu
from jax.sharding import PartitionSpec as P

NLON = 3088
BASE = 16
LANES = 128
ORDER = {2: (1,), 4: (2, 3, 1), 8: (6, 7, 4, 5, 2, 3, 1)}
GROUPS = {2: ((0,), (1,)), 4: ((0, 1), (2, 3)), 8: ((0, 1, 2, 3), (6, 7), (4, 5))}

F32 = jnp.float32
BF16 = jnp.bfloat16

VMEM = pl.BlockSpec(memory_space=pltpu.VMEM)
SMEM = pl.BlockSpec(memory_space=pltpu.SMEM)
HBM = pl.BlockSpec(memory_space=pltpu.HBM)


def call(
    body, name, out_shape, in_specs, scratch=(), out_specs=VMEM, flops=0, bytes_accessed=0,
    grant=16 * 1024 * 1024,
):
    return pl.pallas_call(
        body,
        out_shape=out_shape,
        in_specs=in_specs,
        out_specs=out_specs,
        scratch_shapes=scratch,
        name=name,
        cost_estimate=pl.CostEstimate(
            flops=flops, bytes_accessed=bytes_accessed, transcendentals=0
        ),
        compiler_params=pltpu.CompilerParams(vmem_limit_bytes=grant),
    )


def pieces(extent, size):
    return [(first, min(first + size, extent)) for first in range(0, extent, size)]


def message_shape(rows, slots):
    if slots > LANES and slots % LANES == LANES // 2 and rows % 2 == 0:
        lines = rows * (slots // LANES) + rows // 2
        return (-(-lines // 2), 2, LANES)
    return (rows, slots)


def put_message(ref, index, value):
    if len(ref.shape) == len(index) + 2:
        ref[index] = value.astype(BF16)
        return
    rows, slots = value.shape
    lines = [value[:, first : first + LANES] for first in range(0, slots - LANES + 1, LANES)]
    rest = value[:, slots - LANES // 2 :]
    lines.append(jnp.concatenate([rest[: rows // 2], rest[rows // 2 :]], axis=1))
    if lines[-1].shape[0] % 2:
        lines.append(lines[-1][:1])
    lines = jnp.concatenate(lines, axis=0)
    for k in range(lines.shape[0] // 2):
        ref[index + (k,)] = lines[2 * k : 2 * k + 2].astype(BF16)


def get_message(message, rows, slots):
    if message.ndim == 2:
        return message
    lines = jnp.concatenate([message[k] for k in range(message.shape[0])], axis=0)
    whole = slots // LANES
    parts = [lines[k * rows : (k + 1) * rows] for k in range(whole)]
    rest = lines[whole * rows : whole * rows + rows // 2]
    half = LANES // 2
    parts.append(jnp.concatenate([rest[:, :half], rest[:, half:]], axis=0))
    return jnp.concatenate(parts, axis=1)


def turn_kernel(rank_ref, legendre_ref, *refs):
    *out_refs, turned_ref = refs
    for first, last in pieces(legendre_ref.shape[1], LANES):
        turned_ref[first:last, :] = legendre_ref[:, first:last].T
    degrees = turned_ref.shape[0] // len(out_refs)
    for d, out_ref in enumerate(out_refs):
        start = (rank_ref[0] ^ d) * degrees
        if degrees % 16 == 0:
            start = pl.multiple_of(start, 16)
        out_ref[...] = turned_ref[pl.ds(start, degrees), :]


def turn_all_kernel(legendre_ref, out_ref):
    for first, last in pieces(legendre_ref.shape[1], LANES):
        out_ref[first:last, :] = legendre_ref[:, first:last].T


def turn_spectra_kernel(repeats, fields, rank_ref, spectra_ref, ids_ref, out_ref):
    count, slots, degrees = spectra_ref.shape
    levels = count // (2 * fields)
    degree = rank_ref[0] * degrees + lax.broadcasted_iota(jnp.int32, (degrees, slots), 0)
    alive = degree >= ids_ref[...]
    for i in range(count):
        field, level, part = i // (2 * levels), (i // 2) % levels, i % 2
        turned = jnp.where(alive, spectra_ref[i].astype(F32).T, 0.0)
        place = (level * fields + field) * 2 + part
        out_ref[place] = jnp.concatenate([turned] * repeats, axis=1)


def forward_sums(legendre_refs, spectra_ref):
    degrees, columns = legendre_refs[0].shape
    fields = spectra_ref.shape[0]
    tiles = [[] for _ in legendre_refs]
    for left, right in pieces(columns, LANES):
        sums = [[None] * fields for _ in legendre_refs]
        for first, last in pieces(degrees, 16):
            own = [ref[first:last, left:right].astype(F32) for ref in legendre_refs]
            for i in range(fields):
                other = spectra_ref[i, first:last, left:right]
                for k, value in enumerate(own):
                    product = value * other
                    if last - first == 16:
                        product = product[:8] + product[8:]
                    else:
                        product = jnp.sum(product, axis=0, keepdims=True)
                    sums[k][i] = product if sums[k][i] is None else sums[k][i] + product
        for tile, values in zip(tiles, sums):
            rows = [jnp.sum(value, axis=0, keepdims=True) for value in values]
            tile.append(jnp.concatenate(rows, axis=0))
    return [jnp.concatenate(tile, axis=1) for tile in tiles]


def early_forward_kernel(spectra_ref, *refs):
    *legendre_refs, out_ref = refs
    for first, last in pieces(len(legendre_refs), 2):
        for k, value in enumerate(forward_sums(legendre_refs[first:last], spectra_ref)):
            out_ref[first + k] = value


def put_row_messages(levels, owned, slots, out_ref, a, value):
    per_level = value.shape[0] // levels
    rows = value.shape[1] // slots * levels
    for row in range(rows):
        lat, level = row // levels, row % levels
        message = value[
            level * per_level : (level + 1) * per_level, lat * slots : (lat + 1) * slots
        ]
        put_message(out_ref, (a * (rows // owned) + row // owned, row % owned), message)


def last_forward_kernel(levels, owned, slots, groups, rank_ref, spectra_ref, *refs):
    *early_refs, out_ref = refs[: len(groups) - 1] + refs[-1:]
    legendre_refs = refs[len(groups) - 1 : -1]
    put = functools.partial(put_row_messages, levels, owned, slots, out_ref)
    for places, ref in zip(groups[:-1], early_refs):
        for k, d in enumerate(places):
            put(rank_ref[0] ^ d, ref[k])
    for first, last in pieces(len(legendre_refs), 2):
        values = forward_sums(legendre_refs[first:last], spectra_ref)
        for d, value in zip(groups[-1][first:last], values):
            put(rank_ref[0] ^ d, value)


def loop_forward_kernel(levels, owned, slots, spectra_ref, legendre_ref, out_ref):
    def one_source(a, carry):
        (value,) = forward_sums([legendre_ref.at[a]], spectra_ref)
        put_row_messages(levels, owned, slots, out_ref, a, value)
        return carry

    lax.fori_loop(0, legendre_ref.shape[0], one_source, 0)


def cos_sin(places, ids, count, inverse):
    quads = 4.0 * places * ids
    turns = jnp.floor(quads * inverse + 0.5)
    angle = (quads - turns * count) * (inverse * (math.pi / 2))
    square = angle * angle
    c = 1.0 + square * (-1 / 2 + square * (1 / 24 + square * (-1 / 720 + square * (1 / 40320))))
    s = angle * (
        1.0 + square * (-1 / 6 + square * (1 / 120 + square * (-1 / 5040 + square * (1 / 362880))))
    )
    quadrant = turns - 4.0 * jnp.floor(turns * 0.25)
    odd = (quadrant == 1.0) | (quadrant == 3.0)
    cosine = jnp.where(odd, s, c)
    sine = jnp.where(odd, c, s)
    cosine = jnp.where((quadrant == 1.0) | (quadrant == 2.0), -cosine, cosine)
    sine = jnp.where(quadrant >= 2.0, -sine, sine)
    return cosine, sine


def image_signs(ids):
    quadrant = ids - 4.0 * jnp.floor(ids * 0.25)
    one = jnp.ones_like(ids)
    none = jnp.zeros_like(ids)
    parity = jnp.where((quadrant == 1.0) | (quadrant == 3.0), -1.0, 1.0)
    c = jnp.where(quadrant == 0.0, 1.0, jnp.where(quadrant == 2.0, -1.0, 0.0))
    s = jnp.where(quadrant == 1.0, 1.0, jnp.where(quadrant == 3.0, -1.0, 0.0))
    cos_cos = [one, one, parity, parity, c, c, c, c]
    cos_sin = [none, none, none, none, s, -s, -s, s]
    sin_cos = [none, none, none, none, s, s, -s, -s]
    sin_sin = [one, -one, -parity, parity, -c, c, -c, c]
    return [jnp.concatenate(rows, axis=0) for rows in (cos_cos, cos_sin, sin_cos, sin_sin)]


def table_kernel(
    levels, rank_ref, nlon_ref, coriolis_ref, weight_ref, ids_ref,
    table_ref, left_ref, right_ref, share_ref, rotation_ref, base_ref, step_ref,
):
    owned = table_ref.shape[0]
    steps = step_ref.shape[1]
    waves = ids_ref.shape[1]
    ids = ids_ref[...].astype(F32)
    signs = image_signs(ids)
    for offset in range(owned):
        latitude = (rank_ref[0] * owned + offset) // levels
        count_int = nlon_ref[latitude]
        count = jnp.full((1, waves), count_int.astype(F32))
        inverse = 1.0 / count
        rows = lax.broadcasted_iota(jnp.int32, (BASE, waves), 0).astype(F32)
        base_ref[0], base_ref[1] = cos_sin(rows, ids, count, inverse)
        rows = lax.broadcasted_iota(jnp.int32, (steps, waves), 0).astype(F32) * BASE
        step_ref[0], step_ref[1] = cos_sin(rows, ids, count, inverse)
        for a in range(steps):
            step_c = step_ref[0, a : a + 1, :]
            step_s = step_ref[1, a : a + 1, :]
            base_c = base_ref[0]
            base_s = base_ref[1]
            here = slice(a * BASE, (a + 1) * BASE)
            table_ref[offset, here, :waves] = (step_c * base_c - step_s * base_s).astype(BF16)
            table_ref[offset, here, waves:] = (step_s * base_c + step_c * base_s).astype(BF16)

        factor = jnp.where(ids == 0.0, 1.0, 2.0)
        factor = jnp.where(2.0 * ids < count, factor, 0.0)
        scale = jnp.where(factor > 0.0, weight_ref[latitude] / count, 0.0)
        left_ref[offset, 0] = signs[0] * factor
        left_ref[offset, 1] = -signs[2] * factor
        left_ref[offset, 2] = signs[1] * factor
        left_ref[offset, 3] = -signs[3] * factor
        right_ref[offset, 0] = signs[0] * scale
        right_ref[offset, 1] = signs[1] * scale
        right_ref[offset, 2] = -signs[2] * scale
        right_ref[offset, 3] = -signs[3] * scale
        place = lax.broadcasted_iota(jnp.int32, share_ref.shape[1:], 1)
        share = jnp.where((place == 0) | (8 * place == count_int), 0.5, 1.0)
        share_ref[offset] = jnp.where(8 * place <= count_int, share, 0.0)
        rotation_ref[offset] = jnp.full(rotation_ref.shape[1:], coriolis_ref[latitude])


def grid_kernel(
    slots, partial_ref, table_ref, left_ref, right_ref, share_ref, rotation_ref, out_ref, rows_ref
):
    owned = partial_ref.shape[1]
    waves = left_ref.shape[-1]
    parts = waves // slots
    sources = partial_ref.shape[0] // parts
    for offset in range(owned):

        def total(w):
            def add(a, value):
                return value + partial_ref[a * parts + w, offset].astype(F32)

            if sources > 8:
                return lax.fori_loop(1, sources, add, partial_ref[w, offset].astype(F32))
            value = partial_ref[w, offset].astype(F32)
            for a in range(1, sources):
                value = add(a, value)
            return value

        fourier = jnp.concatenate(
            [get_message(total(w), 6, slots) for w in range(parts)], axis=1
        )
        fourier = fourier.astype(BF16).astype(F32)
        for field in range(3):
            here = slice(8 * field, 8 * field + 8)
            real = fourier[2 * field : 2 * field + 1]
            imag = fourier[2 * field + 1 : 2 * field + 2]
            rows_ref[here, :waves] = real * left_ref[offset, 0] + imag * left_ref[offset, 1]
            rows_ref[here, waves:] = real * left_ref[offset, 2] + imag * left_ref[offset, 3]
        grid = lax.dot_general(
            rows_ref[...].astype(BF16),
            table_ref[offset],
            (((1,), (1,)), ((), ())),
            preferred_element_type=F32,
        )
        vorticity, divergence, temperature = grid[0:8], grid[8:16], grid[16:24]
        share = share_ref[offset]

        def shared(product):
            rounded = jnp.where(share > 0.0, product, 0.0).astype(BF16)
            return rounded.astype(F32) * share

        stretch = shared(-(vorticity + rotation_ref[offset]) * divergence)
        heating = shared(-temperature * divergence)
        products = jnp.concatenate([stretch, heating], axis=0).astype(BF16)
        sums = jnp.dot(products, table_ref[offset], preferred_element_type=F32)
        both = []
        for q in range(2):
            c = sums[8 * q : 8 * q + 8, :waves]
            s = sums[8 * q : 8 * q + 8, waves:]
            for k in range(2):
                term = c * right_ref[offset, 2 * k] + s * right_ref[offset, 2 * k + 1]
                both.append(jnp.sum(term, axis=0, keepdims=True))
        back = jnp.concatenate(both, axis=0)
        for w in range(parts):
            part = back[:, w * slots : (w + 1) * slots]

            def put(a, carry):
                put_message(out_ref, (a * parts + w, offset), part)
                return carry

            if sources > 8:
                lax.fori_loop(0, sources, put, 0)
            else:
                for a in range(sources):
                    put(a, 0)


def backward_kernel(levels, rank_ref, back_ref, ids_ref, *refs):
    *legendre_refs, out_ref, wide_ref, sums_ref, done_ref, sems = refs
    sources, _, _, columns = wide_ref.shape
    degrees = sums_ref.shape[1]
    outs, slots, _ = out_ref.shape
    lats = columns // slots
    owned = back_ref.shape[1]
    targets = back_ref.shape[0] // sources
    apart = len(legendre_refs) > 1

    def spread(k, a):
        for level in range(levels):
            rows = []
            for lat in range(lats):
                row = lat * levels + level
                rows.append(back_ref[a * targets + row // owned, row % owned].astype(F32))
            both = jnp.concatenate(rows, axis=1)
            for i in range(4):
                place = ((i // 2) * levels + level) * 2 + i % 2
                wide_ref[k, place] = jnp.broadcast_to(both[i : i + 1], (8, columns))

    if apart:
        for d in range(sources):
            spread(d, rank_ref[0] ^ d)
    else:
        lax.fori_loop(0, sources, lambda a, carry: spread(a, a) or carry, 0)

    degree = rank_ref[0] * degrees + lax.broadcasted_iota(jnp.int32, (degrees, slots), 0)
    alive = degree >= ids_ref[...]
    copies = []
    for own in pieces(outs, 4):
        for first, last in pieces(degrees, 16):
            for left, right in pieces(columns, LANES):

                def add(k, piece, sums):
                    piece = piece.astype(F32)
                    added = []
                    for i in range(*own):
                        other = wide_ref[k, i, :, left:right]
                        other = jnp.concatenate([other, other], axis=0)[: last - first]
                        term = piece * other
                        past = sums[i - own[0]]
                        added.append(term if past is None else past + term)
                    return tuple(added)

                count = own[1] - own[0]
                if apart:
                    sums = (None,) * count
                    for k, ref in enumerate(legendre_refs):
                        sums = add(k, ref[first:last, left:right], sums)
                else:
                    sums = lax.fori_loop(
                        0,
                        sources,
                        lambda a, sums: add(a, legendre_refs[0][a, first:last, left:right], sums),
                        (jnp.zeros((last - first, right - left), F32),) * count,
                    )
                for i in range(*own):
                    sums_ref[i, first:last, left:right] = sums[i - own[0]]
        for i in range(*own):
            value = sums_ref[i]
            folded = value[:, :slots]
            for lat in range(1, lats):
                folded = folded + value[:, lat * slots : (lat + 1) * slots]
            done_ref[i] = jnp.where(alive, folded, 0.0).T
            copies.append(pltpu.make_async_copy(done_ref.at[i], out_ref.at[i], sems.at[i]))
            copies[-1].start()
    for copy in copies:
        copy.wait()


def local(n_lat, n_wave, spectra, legendre, wave_m, nlon, coriolis, gauss_quadrature_weight):
    lats, slots, total = legendre.shape
    fields, levels = spectra.shape[:2]
    waves = wave_m.shape[0]
    degrees = spectra.shape[4]
    columns = lats * slots
    owned = lats * levels // n_wave
    lat_rank = lax.axis_index("lat").reshape(1)
    wave_rank = lax.axis_index("wave").reshape(1)
    steps = -(-(NLON // 8 + 1) // BASE)
    places = steps * BASE

    rows = legendre.reshape(columns, total)
    apart = n_lat in (2, 4, 8)
    if apart:
        blocks = call(
            turn_kernel,
            "turn",
            (jax.ShapeDtypeStruct((degrees, columns), BF16),) * n_lat,
            [SMEM, VMEM],
            [pltpu.VMEM((total, columns), BF16)],
            out_specs=(VMEM,) * n_lat,
            bytes_accessed=4 * total * columns,
        )(lat_rank, rows)
        turned = {0: blocks[0]}
        for d in ORDER[n_lat]:
            turned[d] = lax.ppermute(blocks[d], "lat", [(i, i ^ d) for i in range(n_lat)])
    else:
        blocks = call(
            turn_all_kernel,
            "turn",
            jax.ShapeDtypeStruct((total, columns), BF16),
            [VMEM],
            bytes_accessed=4 * total * columns,
        )(rows)
        blocks = lax.all_to_all(blocks.reshape(n_lat, degrees, columns), "lat", 0, 0, tiled=True)
        turned = {0: blocks}

    own_ids = lax.dynamic_slice_in_dim(wave_m, wave_rank[0] * slots, slots, 0).reshape(1, slots)
    all_ids = wave_m.reshape(1, waves)
    spectra_turned = call(
        functools.partial(turn_spectra_kernel, lats, fields),
        "turn_spectra",
        jax.ShapeDtypeStruct((2 * fields * levels, degrees, columns), F32),
        [SMEM, VMEM, VMEM],
        flops=10 * fields * levels * degrees * columns,
        bytes_accessed=8 * fields * levels * degrees * columns,
    )(lat_rank, spectra.reshape(2 * fields * levels, slots, degrees), own_ids)

    row = call(
        functools.partial(table_kernel, levels),
        "table",
        (
            jax.ShapeDtypeStruct((owned, places, 2 * waves), BF16),
            jax.ShapeDtypeStruct((owned, 4, 8, waves), F32),
            jax.ShapeDtypeStruct((owned, 4, 8, waves), F32),
            jax.ShapeDtypeStruct((owned, 8, places), F32),
            jax.ShapeDtypeStruct((owned, 8, places), F32),
        ),
        [SMEM, SMEM, SMEM, SMEM, VMEM],
        [pltpu.VMEM((2, BASE, waves), F32), pltpu.VMEM((2, steps, waves), F32)],
        out_specs=(VMEM,) * 5,
        flops=16 * owned * places * waves,
        bytes_accessed=4 * owned * places * waves,
    )(wave_rank, nlon, coriolis, gauss_quadrature_weight, all_ids)
    spectra_turned, *row = lax.optimization_barrier((spectra_turned, *row))

    message = jax.ShapeDtypeStruct(
        (n_lat * n_wave, owned) + message_shape(2 * fields, slots), BF16
    )
    cost = 4 * fields * levels * degrees * columns
    if apart:
        groups = GROUPS[n_lat]
        early = []
        for part in groups[:-1]:
            early.append(
                call(
                    early_forward_kernel,
                    "early_forward",
                    jax.ShapeDtypeStruct((len(part), 2 * fields * levels, columns), F32),
                    [VMEM] * (1 + len(part)),
                    flops=len(part) * cost,
                    bytes_accessed=cost,
                )(spectra_turned, *[turned[d] for d in part])
            )
        partial = call(
            functools.partial(last_forward_kernel, levels, owned, slots, groups),
            "forward",
            message,
            [SMEM] + [VMEM] * (len(groups) + len(groups[-1])),
            flops=len(groups[-1]) * cost,
            bytes_accessed=cost,
        )(lat_rank, spectra_turned, *early, *[turned[d] for d in groups[-1]])
    else:
        partial = call(
            functools.partial(loop_forward_kernel, levels, owned, slots),
            "forward",
            message,
            [VMEM, VMEM],
            flops=n_lat * cost,
            bytes_accessed=cost,
        )(spectra_turned, turned[0])
    partial = lax.all_to_all(partial, ("lat", "wave"), 0, 0, tiled=True)

    back = call(
        functools.partial(grid_kernel, slots),
        "grid",
        jax.ShapeDtypeStruct((n_lat * n_wave, owned, 4, slots), BF16),
        [VMEM] * 6,
        [pltpu.VMEM((24, 2 * waves), F32)],
        flops=128 * owned * places * waves,
        bytes_accessed=4 * owned * places * waves,
    )(partial, *row)
    back = lax.all_to_all(back, ("lat", "wave"), 0, 0, tiled=True)

    outs = 4 * levels
    out = call(
        functools.partial(backward_kernel, levels),
        "backward",
        jax.ShapeDtypeStruct((outs, slots, degrees), F32),
        [SMEM, VMEM, VMEM] + [VMEM] * len(turned),
        [
            pltpu.VMEM((n_lat, outs, 8, columns), F32),
            pltpu.VMEM((outs, degrees, columns), F32),
            pltpu.VMEM((outs, slots, degrees), F32),
            pltpu.SemaphoreType.DMA((outs,)),
        ],
        out_specs=HBM,
        flops=2 * n_lat * outs * degrees * columns,
        bytes_accessed=8 * outs * degrees * slots,
    )(lat_rank, back, own_ids, *[turned[d] for d in sorted(turned)])
    return out.reshape(2, levels, 2, slots, degrees)


def solution(mesh):
    placed = (
        P(None, None, None, "wave", "lat"),
        P("lat", "wave", None),
        P(),
        P("lat"),
        P("lat"),
        P("lat"),
    )
    return jax.shard_map(
        functools.partial(local, mesh.shape["lat"], mesh.shape["wave"]),
        mesh=mesh,
        in_specs=placed,
        out_specs=P(None, None, None, "wave", "lat"),
        check_vma=False,
    )
```

```python
import functools
import math

import jax
import jax.numpy as jnp
from jax import lax
from jax.experimental import pallas as pl
from jax.experimental.pallas import tpu as pltpu
from jax.sharding import PartitionSpec as P

NLON = 3088
BASE = 16
LANES = 128
ORDER = {2: (1,), 4: (2, 3, 1), 8: (6, 7, 4, 5, 2, 3, 1)}
GROUPS = {2: ((0,), (1,)), 4: ((0, 1), (2, 3)), 8: ((0, 1, 2, 3), (6, 7), (4, 5))}

F32 = jnp.float32
BF16 = jnp.bfloat16

VMEM = pl.BlockSpec(memory_space=pltpu.VMEM)
SMEM = pl.BlockSpec(memory_space=pltpu.SMEM)
HBM = pl.BlockSpec(memory_space=pltpu.HBM)


def call(
    body, out_shape, in_specs, scratch=(), out_specs=VMEM, flops=0, bytes_accessed=0,
    grant=16 * 1024 * 1024,
):
    return pl.pallas_call(
        body,
        out_shape=out_shape,
        in_specs=in_specs,
        out_specs=out_specs,
        scratch_shapes=scratch,
        cost_estimate=pl.CostEstimate(
            flops=flops, bytes_accessed=bytes_accessed, transcendentals=0
        ),
        compiler_params=pltpu.CompilerParams(vmem_limit_bytes=grant),
    )


def pieces(extent, size):
    return [(first, min(first + size, extent)) for first in range(0, extent, size)]


def message_shape(rows, slots):
    if slots > LANES and slots % LANES == LANES // 2 and rows % 2 == 0:
        lines = rows * (slots // LANES) + rows // 2
        return (-(-lines // 2), 2, LANES)
    return (rows, slots)


def put_message(ref, index, value):
    if len(ref.shape) == len(index) + 2:
        ref[index] = value.astype(BF16)
        return
    rows, slots = value.shape
    lines = [value[:, first : first + LANES] for first in range(0, slots - LANES + 1, LANES)]
    rest = value[:, slots - LANES // 2 :]
    lines.append(jnp.concatenate([rest[: rows // 2], rest[rows // 2 :]], axis=1))
    if lines[-1].shape[0] % 2:
        lines.append(lines[-1][:1])
    lines = jnp.concatenate(lines, axis=0)
    for k in range(lines.shape[0] // 2):
        ref[index + (k,)] = lines[2 * k : 2 * k + 2].astype(BF16)


def get_message(message, rows, slots):
    if message.ndim == 2:
        return message
    lines = jnp.concatenate([message[k] for k in range(message.shape[0])], axis=0)
    whole = slots // LANES
    parts = [lines[k * rows : (k + 1) * rows] for k in range(whole)]
    rest = lines[whole * rows : whole * rows + rows // 2]
    half = LANES // 2
    parts.append(jnp.concatenate([rest[:, :half], rest[:, half:]], axis=0))
    return jnp.concatenate(parts, axis=1)


def turn_kernel(rank_ref, legendre_ref, *refs):
    *out_refs, turned_ref = refs
    for first, last in pieces(legendre_ref.shape[1], LANES):
        turned_ref[first:last, :] = legendre_ref[:, first:last].T
    degrees = turned_ref.shape[0] // len(out_refs)
    for d, out_ref in enumerate(out_refs):
        start = (rank_ref[0] ^ d) * degrees
        if degrees % 16 == 0:
            start = pl.multiple_of(start, 16)
        out_ref[...] = turned_ref[pl.ds(start, degrees), :]


def turn_all_kernel(legendre_ref, out_ref):
    for first, last in pieces(legendre_ref.shape[1], LANES):
        out_ref[first:last, :] = legendre_ref[:, first:last].T


def turn_spectra_kernel(repeats, fields, rank_ref, spectra_ref, ids_ref, out_ref):
    count, slots, degrees = spectra_ref.shape
    levels = count // (2 * fields)
    degree = rank_ref[0] * degrees + lax.broadcasted_iota(jnp.int32, (degrees, slots), 0)
    alive = degree >= ids_ref[...]
    for i in range(count):
        field, level, part = i // (2 * levels), (i // 2) % levels, i % 2
        turned = jnp.where(alive, spectra_ref[i].astype(F32).T, 0.0)
        place = (level * fields + field) * 2 + part
        out_ref[place] = jnp.concatenate([turned] * repeats, axis=1)


def forward_sums(legendre_refs, spectra_ref):
    degrees, columns = legendre_refs[0].shape
    fields = spectra_ref.shape[0]
    tiles = [[] for _ in legendre_refs]
    for left, right in pieces(columns, LANES):
        sums = [[None] * fields for _ in legendre_refs]
        for first, last in pieces(degrees, 16):
            own = [ref[first:last, left:right].astype(F32) for ref in legendre_refs]
            for i in range(fields):
                other = spectra_ref[i, first:last, left:right]
                for k, value in enumerate(own):
                    product = value * other
                    if last - first == 16:
                        product = product[:8] + product[8:]
                    else:
                        product = jnp.sum(product, axis=0, keepdims=True)
                    sums[k][i] = product if sums[k][i] is None else sums[k][i] + product
        for tile, values in zip(tiles, sums):
            rows = [jnp.sum(value, axis=0, keepdims=True) for value in values]
            tile.append(jnp.concatenate(rows, axis=0))
    return [jnp.concatenate(tile, axis=1) for tile in tiles]


def early_forward_kernel(spectra_ref, *refs):
    *legendre_refs, out_ref = refs
    for first, last in pieces(len(legendre_refs), 2):
        for k, value in enumerate(forward_sums(legendre_refs[first:last], spectra_ref)):
            out_ref[first + k] = value


def put_row_messages(levels, owned, slots, out_ref, a, value):
    per_level = value.shape[0] // levels
    rows = value.shape[1] // slots * levels
    for row in range(rows):
        lat, level = row // levels, row % levels
        message = value[
            level * per_level : (level + 1) * per_level, lat * slots : (lat + 1) * slots
        ]
        put_message(out_ref, (a * (rows // owned) + row // owned, row % owned), message)


def last_forward_kernel(levels, owned, slots, groups, rank_ref, spectra_ref, *refs):
    *early_refs, out_ref = refs[: len(groups) - 1] + refs[-1:]
    legendre_refs = refs[len(groups) - 1 : -1]
    put = functools.partial(put_row_messages, levels, owned, slots, out_ref)
    for places, ref in zip(groups[:-1], early_refs):
        for k, d in enumerate(places):
            put(rank_ref[0] ^ d, ref[k])
    for first, last in pieces(len(legendre_refs), 2):
        values = forward_sums(legendre_refs[first:last], spectra_ref)
        for d, value in zip(groups[-1][first:last], values):
            put(rank_ref[0] ^ d, value)


def loop_forward_kernel(levels, owned, slots, spectra_ref, legendre_ref, out_ref):
    def one_source(a, carry):
        (value,) = forward_sums([legendre_ref.at[a]], spectra_ref)
        put_row_messages(levels, owned, slots, out_ref, a, value)
        return carry

    lax.fori_loop(0, legendre_ref.shape[0], one_source, 0)


def cos_sin(places, ids, count, inverse):
    quads = 4.0 * places * ids
    turns = jnp.floor(quads * inverse + 0.5)
    angle = (quads - turns * count) * (inverse * (math.pi / 2))
    square = angle * angle
    c = 1.0 + square * (-1 / 2 + square * (1 / 24 + square * (-1 / 720 + square * (1 / 40320))))
    s = angle * (
        1.0 + square * (-1 / 6 + square * (1 / 120 + square * (-1 / 5040 + square * (1 / 362880))))
    )
    quadrant = turns - 4.0 * jnp.floor(turns * 0.25)
    odd = (quadrant == 1.0) | (quadrant == 3.0)
    cosine = jnp.where(odd, s, c)
    sine = jnp.where(odd, c, s)
    cosine = jnp.where((quadrant == 1.0) | (quadrant == 2.0), -cosine, cosine)
    sine = jnp.where(quadrant >= 2.0, -sine, sine)
    return cosine, sine


def image_signs(ids):
    quadrant = ids - 4.0 * jnp.floor(ids * 0.25)
    one = jnp.ones_like(ids)
    none = jnp.zeros_like(ids)
    parity = jnp.where((quadrant == 1.0) | (quadrant == 3.0), -1.0, 1.0)
    c = jnp.where(quadrant == 0.0, 1.0, jnp.where(quadrant == 2.0, -1.0, 0.0))
    s = jnp.where(quadrant == 1.0, 1.0, jnp.where(quadrant == 3.0, -1.0, 0.0))
    cos_cos = [one, one, parity, parity, c, c, c, c]
    cos_sin = [none, none, none, none, s, -s, -s, s]
    sin_cos = [none, none, none, none, s, s, -s, -s]
    sin_sin = [one, -one, -parity, parity, -c, c, -c, c]
    return [jnp.concatenate(rows, axis=0) for rows in (cos_cos, cos_sin, sin_cos, sin_sin)]


def table_kernel(
    levels, rank_ref, nlon_ref, coriolis_ref, weight_ref, ids_ref,
    table_ref, left_ref, right_ref, share_ref, rotation_ref, base_ref, step_ref,
):
    owned = table_ref.shape[0]
    steps = step_ref.shape[1]
    waves = ids_ref.shape[1]
    ids = ids_ref[...].astype(F32)
    signs = image_signs(ids)
    for offset in range(owned):
        latitude = (rank_ref[0] * owned + offset) // levels
        count_int = nlon_ref[latitude]
        count = jnp.full((1, waves), count_int.astype(F32))
        inverse = 1.0 / count
        rows = lax.broadcasted_iota(jnp.int32, (BASE, waves), 0).astype(F32)
        base_ref[0], base_ref[1] = cos_sin(rows, ids, count, inverse)
        rows = lax.broadcasted_iota(jnp.int32, (steps, waves), 0).astype(F32) * BASE
        step_ref[0], step_ref[1] = cos_sin(rows, ids, count, inverse)
        for a in range(steps):
            step_c = step_ref[0, a : a + 1, :]
            step_s = step_ref[1, a : a + 1, :]
            base_c = base_ref[0]
            base_s = base_ref[1]
            here = slice(a * BASE, (a + 1) * BASE)
            table_ref[offset, here, :waves] = (step_c * base_c - step_s * base_s).astype(BF16)
            table_ref[offset, here, waves:] = (step_s * base_c + step_c * base_s).astype(BF16)

        factor = jnp.where(ids == 0.0, 1.0, 2.0)
        factor = jnp.where(2.0 * ids < count, factor, 0.0)
        scale = jnp.where(factor > 0.0, weight_ref[latitude] / count, 0.0)
        left_ref[offset, 0] = signs[0] * factor
        left_ref[offset, 1] = -signs[2] * factor
        left_ref[offset, 2] = signs[1] * factor
        left_ref[offset, 3] = -signs[3] * factor
        right_ref[offset, 0] = signs[0] * scale
        right_ref[offset, 1] = signs[1] * scale
        right_ref[offset, 2] = -signs[2] * scale
        right_ref[offset, 3] = -signs[3] * scale
        place = lax.broadcasted_iota(jnp.int32, share_ref.shape[1:], 1)
        share = jnp.where((place == 0) | (8 * place == count_int), 0.5, 1.0)
        share_ref[offset] = jnp.where(8 * place <= count_int, share, 0.0)
        rotation_ref[offset] = jnp.full(rotation_ref.shape[1:], coriolis_ref[latitude])


def grid_kernel(
    slots, partial_ref, table_ref, left_ref, right_ref, share_ref, rotation_ref, out_ref, rows_ref
):
    owned = partial_ref.shape[1]
    waves = left_ref.shape[-1]
    parts = waves // slots
    sources = partial_ref.shape[0] // parts
    for offset in range(owned):

        def total(w):
            def add(a, value):
                return value + partial_ref[a * parts + w, offset].astype(F32)

            if sources > 8:
                return lax.fori_loop(1, sources, add, partial_ref[w, offset].astype(F32))
            value = partial_ref[w, offset].astype(F32)
            for a in range(1, sources):
                value = add(a, value)
            return value

        fourier = jnp.concatenate(
            [get_message(total(w), 6, slots) for w in range(parts)], axis=1
        )
        fourier = fourier.astype(BF16).astype(F32)
        for field in range(3):
            here = slice(8 * field, 8 * field + 8)
            real = fourier[2 * field : 2 * field + 1]
            imag = fourier[2 * field + 1 : 2 * field + 2]
            rows_ref[here, :waves] = real * left_ref[offset, 0] + imag * left_ref[offset, 1]
            rows_ref[here, waves:] = real * left_ref[offset, 2] + imag * left_ref[offset, 3]
        grid = lax.dot_general(
            rows_ref[...].astype(BF16),
            table_ref[offset],
            (((1,), (1,)), ((), ())),
            preferred_element_type=F32,
        )
        vorticity, divergence, temperature = grid[0:8], grid[8:16], grid[16:24]
        share = share_ref[offset]

        def shared(product):
            rounded = jnp.where(share > 0.0, product, 0.0).astype(BF16)
            return rounded.astype(F32) * share

        stretch = shared(-(vorticity + rotation_ref[offset]) * divergence)
        heating = shared(-temperature * divergence)
        products = jnp.concatenate([stretch, heating], axis=0).astype(BF16)
        sums = jnp.dot(products, table_ref[offset], preferred_element_type=F32)
        both = []
        for q in range(2):
            c = sums[8 * q : 8 * q + 8, :waves]
            s = sums[8 * q : 8 * q + 8, waves:]
            for k in range(2):
                term = c * right_ref[offset, 2 * k] + s * right_ref[offset, 2 * k + 1]
                both.append(jnp.sum(term, axis=0, keepdims=True))
        back = jnp.concatenate(both, axis=0)
        for w in range(parts):
            part = back[:, w * slots : (w + 1) * slots]

            def put(a, carry):
                put_message(out_ref, (a * parts + w, offset), part)
                return carry

            if sources > 8:
                lax.fori_loop(0, sources, put, 0)
            else:
                for a in range(sources):
                    put(a, 0)


def backward_kernel(levels, rank_ref, back_ref, ids_ref, *refs):
    *legendre_refs, out_ref, wide_ref, sums_ref, done_ref, sems = refs
    sources, _, _, columns = wide_ref.shape
    degrees = sums_ref.shape[1]
    outs, slots, _ = out_ref.shape
    lats = columns // slots
    owned = back_ref.shape[1]
    targets = back_ref.shape[0] // sources
    apart = len(legendre_refs) > 1

    def spread(k, a):
        for level in range(levels):
            rows = []
            for lat in range(lats):
                row = lat * levels + level
                rows.append(back_ref[a * targets + row // owned, row % owned].astype(F32))
            both = jnp.concatenate(rows, axis=1)
            for i in range(4):
                place = ((i // 2) * levels + level) * 2 + i % 2
                wide_ref[k, place] = jnp.broadcast_to(both[i : i + 1], (8, columns))

    if apart:
        for d in range(sources):
            spread(d, rank_ref[0] ^ d)
    else:
        lax.fori_loop(0, sources, lambda a, carry: spread(a, a) or carry, 0)

    degree = rank_ref[0] * degrees + lax.broadcasted_iota(jnp.int32, (degrees, slots), 0)
    alive = degree >= ids_ref[...]
    copies = []
    for own in pieces(outs, outs):
        for first, last in pieces(degrees, 16):
            for left, right in pieces(columns, LANES):

                def add(k, piece, sums):
                    piece = piece.astype(F32)
                    added = []
                    for i in range(*own):
                        other = wide_ref[k, i, :, left:right]
                        other = jnp.concatenate([other, other], axis=0)[: last - first]
                        term = piece * other
                        past = sums[i - own[0]]
                        added.append(term if past is None else past + term)
                    return tuple(added)

                count = own[1] - own[0]
                if apart:
                    sums = (None,) * count
                    for k, ref in enumerate(legendre_refs):
                        sums = add(k, ref[first:last, left:right], sums)
                else:
                    sums = lax.fori_loop(
                        0,
                        sources,
                        lambda a, sums: add(a, legendre_refs[0][a, first:last, left:right], sums),
                        (jnp.zeros((last - first, right - left), F32),) * count,
                    )
                for i in range(*own):
                    sums_ref[i, first:last, left:right] = sums[i - own[0]]
        for i in range(*own):
            value = sums_ref[i]
            folded = value[:, :slots]
            for lat in range(1, lats):
                folded = folded + value[:, lat * slots : (lat + 1) * slots]
            done_ref[i] = jnp.where(alive, folded, 0.0).T
            copies.append(pltpu.make_async_copy(done_ref.at[i], out_ref.at[i], sems.at[i]))
            copies[-1].start()
    for copy in copies:
        copy.wait()


def local(n_lat, n_wave, spectra, legendre, wave_m, nlon, coriolis, gauss_quadrature_weight):
    lats, slots, total = legendre.shape
    fields, levels = spectra.shape[:2]
    waves = wave_m.shape[0]
    degrees = spectra.shape[4]
    columns = lats * slots
    owned = lats * levels // n_wave
    lat_rank = lax.axis_index("lat").reshape(1)
    wave_rank = lax.axis_index("wave").reshape(1)
    steps = -(-(NLON // 8 + 1) // BASE)
    places = steps * BASE

    rows = legendre.reshape(columns, total)
    apart = n_lat in (2, 4, 8)
    if apart:
        blocks = call(
            turn_kernel,
            (jax.ShapeDtypeStruct((degrees, columns), BF16),) * n_lat,
            [SMEM, VMEM],
            [pltpu.VMEM((total, columns), BF16)],
            out_specs=(VMEM,) * n_lat,
            bytes_accessed=4 * total * columns,
        )(lat_rank, rows)
        turned = {0: blocks[0]}
        for d in ORDER[n_lat]:
            turned[d] = lax.ppermute(blocks[d], "lat", [(i, i ^ d) for i in range(n_lat)])
    else:
        blocks = call(
            turn_all_kernel,
            jax.ShapeDtypeStruct((total, columns), BF16),
            [VMEM],
            bytes_accessed=4 * total * columns,
        )(rows)
        blocks = lax.all_to_all(blocks.reshape(n_lat, degrees, columns), "lat", 0, 0, tiled=True)
        turned = {0: blocks}

    own_ids = lax.dynamic_slice_in_dim(wave_m, wave_rank[0] * slots, slots, 0).reshape(1, slots)
    all_ids = wave_m.reshape(1, waves)
    spectra_turned = call(
        functools.partial(turn_spectra_kernel, lats, fields),
        jax.ShapeDtypeStruct((2 * fields * levels, degrees, columns), F32),
        [SMEM, VMEM, VMEM],
        flops=10 * fields * levels * degrees * columns,
        bytes_accessed=8 * fields * levels * degrees * columns,
    )(lat_rank, spectra.reshape(2 * fields * levels, slots, degrees), own_ids)

    row = call(
        functools.partial(table_kernel, levels),
        (
            jax.ShapeDtypeStruct((owned, places, 2 * waves), BF16),
            jax.ShapeDtypeStruct((owned, 4, 8, waves), F32),
            jax.ShapeDtypeStruct((owned, 4, 8, waves), F32),
            jax.ShapeDtypeStruct((owned, 8, places), F32),
            jax.ShapeDtypeStruct((owned, 8, places), F32),
        ),
        [SMEM, SMEM, SMEM, SMEM, VMEM],
        [pltpu.VMEM((2, BASE, waves), F32), pltpu.VMEM((2, steps, waves), F32)],
        out_specs=(VMEM,) * 5,
        flops=16 * owned * places * waves,
        bytes_accessed=4 * owned * places * waves,
    )(wave_rank, nlon, coriolis, gauss_quadrature_weight, all_ids)
    spectra_turned, *row = lax.optimization_barrier((spectra_turned, *row))

    message = jax.ShapeDtypeStruct(
        (n_lat * n_wave, owned) + message_shape(2 * fields, slots), BF16
    )
    cost = 4 * fields * levels * degrees * columns
    if apart:
        groups = GROUPS[n_lat]
        early = []
        for part in groups[:-1]:
            early.append(
                call(
                    early_forward_kernel,
                    jax.ShapeDtypeStruct((len(part), 2 * fields * levels, columns), F32),
                    [VMEM] * (1 + len(part)),
                    flops=len(part) * cost,
                    bytes_accessed=cost,
                )(spectra_turned, *[turned[d] for d in part])
            )
        partial = call(
            functools.partial(last_forward_kernel, levels, owned, slots, groups),
            message,
            [SMEM] + [VMEM] * (len(groups) + len(groups[-1])),
            flops=len(groups[-1]) * cost,
            bytes_accessed=cost,
        )(lat_rank, spectra_turned, *early, *[turned[d] for d in groups[-1]])
    else:
        partial = call(
            functools.partial(loop_forward_kernel, levels, owned, slots),
            message,
            [VMEM, VMEM],
            flops=n_lat * cost,
            bytes_accessed=cost,
        )(spectra_turned, turned[0])
    partial = lax.all_to_all(partial, ("lat", "wave"), 0, 0, tiled=True)

    back = call(
        functools.partial(grid_kernel, slots),
        jax.ShapeDtypeStruct((n_lat * n_wave, owned, 4, slots), BF16),
        [VMEM] * 6,
        [pltpu.VMEM((24, 2 * waves), F32)],
        flops=128 * owned * places * waves,
        bytes_accessed=4 * owned * places * waves,
    )(partial, *row)
    back = lax.all_to_all(back, ("lat", "wave"), 0, 0, tiled=True)

    outs = 4 * levels
    out = call(
        functools.partial(backward_kernel, levels),
        jax.ShapeDtypeStruct((outs, slots, degrees), F32),
        [SMEM, VMEM, VMEM] + [VMEM] * len(turned),
        [
            pltpu.VMEM((n_lat, outs, 8, columns), F32),
            pltpu.VMEM((outs, degrees, columns), F32),
            pltpu.VMEM((outs, slots, degrees), F32),
            pltpu.SemaphoreType.DMA((outs,)),
        ],
        out_specs=HBM,
        flops=2 * n_lat * outs * degrees * columns,
        bytes_accessed=8 * outs * degrees * slots,
    )(lat_rank, back, own_ids, *[turned[d] for d in sorted(turned)])
    return out.reshape(2, levels, 2, slots, degrees)


def solution(mesh):
    placed = (
        P(None, None, None, "wave", "lat"),
        P("lat", "wave", None),
        P(),
        P("lat"),
        P("lat"),
        P("lat"),
    )
    n_lat = mesh.shape["lat"]
    return jax.shard_map(
        functools.partial(local, n_lat, mesh.shape["wave"]),
        mesh=mesh,
        in_specs=placed,
        out_specs=P(None, None, None, "wave", "lat"),
        check_vma=False,
    )
```

```python
import functools
import math

import jax
import jax.numpy as jnp
from jax import lax
from jax.experimental import pallas as pl
from jax.experimental.pallas import tpu as pltpu
from jax.sharding import PartitionSpec as P

NLON = 3088
BASE = 16
LANES = 128
WORK = 128
ORDER = {2: (1,), 4: (2, 3, 1), 8: (6, 4, 7, 5, 2, 3, 1)}
GROUPS = {2: ((0,), (1,)), 4: ((0, 1), (2, 3)), 8: ((0, 1, 2, 3), (6, 7), (4,), (5,))}

F32 = jnp.float32
BF16 = jnp.bfloat16

VMEM = pl.BlockSpec(memory_space=pltpu.VMEM)
SMEM = pl.BlockSpec(memory_space=pltpu.SMEM)
HBM = pl.BlockSpec(memory_space=pltpu.HBM)


def call(
    body, out_shape, in_specs, scratch=(), out_specs=VMEM, flops=0, bytes_accessed=0,
    grant=16 * 1024 * 1024,
):
    return pl.pallas_call(
        body,
        out_shape=out_shape,
        in_specs=in_specs,
        out_specs=out_specs,
        scratch_shapes=scratch,
        cost_estimate=pl.CostEstimate(
            flops=flops, bytes_accessed=bytes_accessed, transcendentals=0
        ),
        compiler_params=pltpu.CompilerParams(vmem_limit_bytes=grant),
    )


def far(value):
    return pltpu.with_memory_space_constraint(value, pltpu.HBM)


def pieces(extent, size):
    return [(first, min(first + size, extent)) for first in range(0, extent, size)]


def message_shape(rows, slots):
    if slots > LANES and slots % LANES == LANES // 2 and rows % 2 == 0:
        lines = rows * (slots // LANES) + rows // 2
        return (-(-lines // 2), 2, LANES)
    return (rows, slots)


def put_message(ref, index, value):
    if len(ref.shape) == len(index) + 2:
        ref[index] = value.astype(BF16)
        return
    rows, slots = value.shape
    lines = [value[:, first : first + LANES] for first in range(0, slots - LANES + 1, LANES)]
    rest = value[:, slots - LANES // 2 :]
    lines.append(jnp.concatenate([rest[: rows // 2], rest[rows // 2 :]], axis=1))
    if lines[-1].shape[0] % 2:
        lines.append(lines[-1][:1])
    lines = jnp.concatenate(lines, axis=0)
    for k in range(lines.shape[0] // 2):
        ref[index + (k,)] = lines[2 * k : 2 * k + 2].astype(BF16)


def get_message(message, rows, slots):
    if message.ndim == 2:
        return message
    lines = jnp.concatenate([message[k] for k in range(message.shape[0])], axis=0)
    whole = slots // LANES
    parts = [lines[k * rows : (k + 1) * rows] for k in range(whole)]
    rest = lines[whole * rows : whole * rows + rows // 2]
    half = LANES // 2
    parts.append(jnp.concatenate([rest[:, :half], rest[:, half:]], axis=0))
    return jnp.concatenate(parts, axis=1)


def turn_kernel(rank_ref, legendre_ref, *refs):
    *out_refs, turned_ref = refs
    for first, last in pieces(legendre_ref.shape[1], LANES):
        turned_ref[first:last, :] = legendre_ref[:, first:last].T
    degrees = turned_ref.shape[0] // len(out_refs)
    for d, out_ref in enumerate(out_refs):
        start = (rank_ref[0] ^ d) * degrees
        if degrees % 16 == 0:
            start = pl.multiple_of(start, 16)
        out_ref[...] = turned_ref[pl.ds(start, degrees), :]


def turn_all_kernel(legendre_ref, out_ref):
    for first, last in pieces(legendre_ref.shape[1], LANES):
        out_ref[first:last, :] = legendre_ref[:, first:last].T


def turn_spectra_kernel(
    repeats, fields, lat_ref, wave_ref, spectra_ref, ids_ref, out_ref, alive_ref
):
    count, slots, degrees = spectra_ref.shape
    levels = count // (2 * fields)
    ids = jnp.zeros((1, slots), jnp.int32)
    for w, (first, last) in enumerate(pieces(ids_ref.shape[1], slots)):
        ids = jnp.where(wave_ref[0] == w, ids_ref[:, first:last], ids)
    degree = lat_ref[0] * degrees + lax.broadcasted_iota(jnp.int32, (degrees, slots), 0)
    alive_ref[...] = jnp.where(degree >= ids, 1.0, 0.0)
    alive = alive_ref[...]
    for i in range(count):
        field, level, part = i // (2 * levels), (i // 2) % levels, i % 2
        turned = spectra_ref[i].astype(F32).T * alive
        place = (level * fields + field) * 2 + part
        out_ref[place] = jnp.concatenate([turned] * repeats, axis=1)


def forward_sums(legendre_refs, spectra_ref):
    degrees, columns = legendre_refs[0].shape
    fields = spectra_ref.shape[0]
    tiles = [[] for _ in legendre_refs]
    for left, right in pieces(columns, LANES):
        sums = [[None] * fields for _ in legendre_refs]
        for first, last in pieces(degrees, 16):
            own = [ref[first:last, left:right].astype(F32) for ref in legendre_refs]
            for i in range(fields):
                other = spectra_ref[i, first:last, left:right]
                for k, value in enumerate(own):
                    product = value * other
                    if last - first == 16:
                        product = product[:8] + product[8:]
                    else:
                        product = jnp.sum(product, axis=0, keepdims=True)
                    sums[k][i] = product if sums[k][i] is None else sums[k][i] + product
        for tile, values in zip(tiles, sums):
            rows = [jnp.sum(value, axis=0, keepdims=True) for value in values]
            tile.append(jnp.concatenate(rows, axis=0))
    return [jnp.concatenate(tile, axis=1) for tile in tiles]


def put_row_messages(levels, owned, slots, out_ref, a, value):
    per_level = value.shape[0] // levels
    rows = value.shape[1] // slots * levels
    for row in range(rows):
        lat, level = row // levels, row % levels
        message = value[
            level * per_level : (level + 1) * per_level, lat * slots : (lat + 1) * slots
        ]
        put_message(out_ref, (a * (rows // owned) + row // owned, row % owned), message)


def early_forward_kernel(levels, owned, slots, spectra_ref, *refs):
    *legendre_refs, out_ref = refs
    for first, last in pieces(len(legendre_refs), 2):
        for k, value in enumerate(forward_sums(legendre_refs[first:last], spectra_ref)):
            put_row_messages(levels, owned, slots, out_ref, first + k, value)


def last_forward_kernel(levels, owned, slots, groups, rank_ref, spectra_ref, *refs):
    *early_refs, out_ref = refs[: len(groups) - 1] + refs[-1:]
    legendre_refs = refs[len(groups) - 1 : -1]
    for places, ref in zip(groups[:-1], early_refs):
        targets = ref.shape[0] // len(places)
        for k, d in enumerate(places):
            start = (rank_ref[0] ^ d) * targets
            out_ref[pl.ds(start, targets)] = ref[k * targets : (k + 1) * targets]
    for first, last in pieces(len(legendre_refs), 2):
        values = forward_sums(legendre_refs[first:last], spectra_ref)
        for d, value in zip(groups[-1][first:last], values):
            put_row_messages(levels, owned, slots, out_ref, rank_ref[0] ^ d, value)


def loop_forward_kernel(levels, owned, slots, spectra_ref, legendre_ref, out_ref):
    def one_source(a, carry):
        (value,) = forward_sums([legendre_ref.at[a]], spectra_ref)
        put_row_messages(levels, owned, slots, out_ref, a, value)
        return carry

    lax.fori_loop(0, legendre_ref.shape[0], one_source, 0)


def cos_sin(places, ids, count, inverse):
    quads = 4.0 * places * ids
    turns = jnp.floor(quads * inverse + 0.5)
    angle = (quads - turns * count) * (inverse * (math.pi / 2))
    square = angle * angle
    c = 1.0 + square * (-1 / 2 + square * (1 / 24 + square * (-1 / 720 + square * (1 / 40320))))
    s = angle * (
        1.0 + square * (-1 / 6 + square * (1 / 120 + square * (-1 / 5040 + square * (1 / 362880))))
    )
    quadrant = turns - 4.0 * jnp.floor(turns * 0.25)
    odd = (quadrant == 1.0) | (quadrant == 3.0)
    cosine = jnp.where(odd, s, c)
    sine = jnp.where(odd, c, s)
    cosine = jnp.where((quadrant == 1.0) | (quadrant == 2.0), -cosine, cosine)
    sine = jnp.where(quadrant >= 2.0, -sine, sine)
    return cosine, sine


def image_signs(ids):
    quadrant = ids - 4.0 * jnp.floor(ids * 0.25)
    one = jnp.ones_like(ids)
    none = jnp.zeros_like(ids)
    parity = jnp.where((quadrant == 1.0) | (quadrant == 3.0), -1.0, 1.0)
    c = jnp.where(quadrant == 0.0, 1.0, jnp.where(quadrant == 2.0, -1.0, 0.0))
    s = jnp.where(quadrant == 1.0, 1.0, jnp.where(quadrant == 3.0, -1.0, 0.0))
    cos_cos = [one, one, parity, parity, c, c, c, c]
    cos_sin = [none, none, none, none, s, -s, -s, s]
    sin_cos = [none, none, none, none, s, s, -s, -s]
    sin_sin = [one, -one, -parity, parity, -c, c, -c, c]
    return [jnp.concatenate(rows, axis=0) for rows in (cos_cos, cos_sin, sin_cos, sin_sin)]


def table_kernel(
    levels, rank_ref, ids_ref, nlon_far, coriolis_far, weight_far,
    table_ref, left_ref, right_ref, share_ref, rotation_ref,
    base_ref, step_ref, nlon_ref, coriolis_ref, weight_ref, sems,
):
    copies = [
        pltpu.make_async_copy(far, near, sems.at[i])
        for i, (far, near) in enumerate(
            [(nlon_far, nlon_ref), (coriolis_far, coriolis_ref), (weight_far, weight_ref)]
        )
    ]
    for copy in copies:
        copy.start()
    for copy in copies:
        copy.wait()
    owned = table_ref.shape[0]
    steps = step_ref.shape[1]
    waves = ids_ref.shape[1]
    ids = ids_ref[...].astype(F32)
    signs = image_signs(ids)
    for offset in range(owned):
        latitude = (rank_ref[0] * owned + offset) // levels
        count_int = nlon_ref[latitude]
        count = jnp.full((1, waves), count_int.astype(F32))
        inverse = 1.0 / count
        rows = lax.broadcasted_iota(jnp.int32, (BASE, waves), 0).astype(F32)
        base_ref[0], base_ref[1] = cos_sin(rows, ids, count, inverse)
        rows = lax.broadcasted_iota(jnp.int32, (steps, waves), 0).astype(F32) * BASE
        step_ref[0], step_ref[1] = cos_sin(rows, ids, count, inverse)
        for a in range(steps):
            step_c = step_ref[0, a : a + 1, :]
            step_s = step_ref[1, a : a + 1, :]
            base_c = base_ref[0]
            base_s = base_ref[1]
            here = slice(a * BASE, (a + 1) * BASE)
            table_ref[offset, here, :waves] = (step_c * base_c - step_s * base_s).astype(BF16)
            table_ref[offset, here, waves:] = (step_s * base_c + step_c * base_s).astype(BF16)

        factor = jnp.where(ids == 0.0, 1.0, 2.0)
        factor = jnp.where(2.0 * ids < count, factor, 0.0)
        scale = jnp.where(factor > 0.0, weight_ref[latitude] / count, 0.0)
        left_ref[offset, 0] = signs[0] * factor
        left_ref[offset, 1] = -signs[2] * factor
        left_ref[offset, 2] = signs[1] * factor
        left_ref[offset, 3] = -signs[3] * factor
        right_ref[offset, 0] = signs[0] * scale
        right_ref[offset, 1] = signs[1] * scale
        right_ref[offset, 2] = -signs[2] * scale
        right_ref[offset, 3] = -signs[3] * scale
        place = lax.broadcasted_iota(jnp.int32, share_ref.shape[1:], 1)
        share = jnp.where((place == 0) | (8 * place == count_int), 0.5, 1.0)
        share_ref[offset] = jnp.where(8 * place <= count_int, share, 0.0)
        rotation_ref[offset] = jnp.full(rotation_ref.shape[1:], coriolis_ref[latitude])


def grid_kernel(
    slots, partial_ref, table_ref, left_ref, right_ref, share_ref, rotation_ref, out_ref, rows_ref
):
    owned = partial_ref.shape[1]
    waves = left_ref.shape[-1]
    parts = waves // slots
    sources = partial_ref.shape[0] // parts
    for offset in range(owned):

        def total(w):
            def add(a, value):
                return value + partial_ref[a * parts + w, offset].astype(F32)

            if sources > 8:
                return lax.fori_loop(1, sources, add, partial_ref[w, offset].astype(F32))
            value = partial_ref[w, offset].astype(F32)
            for a in range(1, sources):
                value = add(a, value)
            return value

        fourier = jnp.concatenate(
            [get_message(total(w), 6, slots) for w in range(parts)], axis=1
        )
        fourier = fourier.astype(BF16).astype(F32)
        for field in range(3):
            here = slice(8 * field, 8 * field + 8)
            real = fourier[2 * field : 2 * field + 1]
            imag = fourier[2 * field + 1 : 2 * field + 2]
            rows_ref[here, :waves] = real * left_ref[offset, 0] + imag * left_ref[offset, 1]
            rows_ref[here, waves:] = real * left_ref[offset, 2] + imag * left_ref[offset, 3]
        grid = lax.dot_general(
            rows_ref[...].astype(BF16),
            table_ref[offset],
            (((1,), (1,)), ((), ())),
            preferred_element_type=F32,
        )
        vorticity, divergence, temperature = grid[0:8], grid[8:16], grid[16:24]
        share = share_ref[offset]

        def shared(product):
            rounded = jnp.where(share > 0.0, product, 0.0).astype(BF16)
            return rounded.astype(F32) * share

        stretch = shared(-(vorticity + rotation_ref[offset]) * divergence)
        heating = shared(-temperature * divergence)
        products = jnp.concatenate([stretch, heating], axis=0).astype(BF16)
        sums = jnp.dot(products, table_ref[offset], preferred_element_type=F32)
        both = []
        for q in range(2):
            c = sums[8 * q : 8 * q + 8, :waves]
            s = sums[8 * q : 8 * q + 8, waves:]
            for k in range(2):
                term = c * right_ref[offset, 2 * k] + s * right_ref[offset, 2 * k + 1]
                both.append(jnp.sum(term, axis=0, keepdims=True))
        back = jnp.concatenate(both, axis=0)
        for w in range(parts):
            part = back[:, w * slots : (w + 1) * slots]

            def put(a, carry):
                put_message(out_ref, (a * parts + w, offset), part)
                return carry

            if sources > 8:
                lax.fori_loop(0, sources, put, 0)
            else:
                for a in range(sources):
                    put(a, 0)


def backward_kernel(levels, rank_ref, back_ref, alive_ref, *refs):
    *legendre_refs, out_ref, wide_ref, sums_ref, done_ref, sems = refs
    sources, _, _, columns = wide_ref.shape
    degrees = sums_ref.shape[1]
    outs, slots, _ = out_ref.shape
    lats = columns // slots
    owned = back_ref.shape[1]
    targets = back_ref.shape[0] // sources
    apart = len(legendre_refs) > 1

    def spread(k, a):
        for level in range(levels):
            rows = []
            for lat in range(lats):
                row = lat * levels + level
                rows.append(back_ref[a * targets + row // owned, row % owned].astype(F32))
            both = jnp.concatenate(rows, axis=1)
            for i in range(4):
                place = ((i // 2) * levels + level) * 2 + i % 2
                wide_ref[k, place] = jnp.broadcast_to(both[i : i + 1], (8, columns))

    if apart:
        for d in range(sources):
            spread(d, rank_ref[0] ^ d)
    else:
        lax.fori_loop(0, sources, lambda a, carry: spread(a, a) or carry, 0)

    alive = alive_ref[...]
    copies = []
    for own in pieces(outs, outs):
        for first, last in pieces(degrees, 16):
            for left, right in pieces(columns, LANES):

                def add(k, piece, sums):
                    piece = piece.astype(F32)
                    added = []
                    for i in range(*own):
                        other = wide_ref[k, i, :, left:right]
                        other = jnp.concatenate([other, other], axis=0)[: last - first]
                        term = piece * other
                        past = sums[i - own[0]]
                        added.append(term if past is None else past + term)
                    return tuple(added)

                count = own[1] - own[0]
                if apart:
                    sums = (None,) * count
                    for k, ref in enumerate(legendre_refs):
                        sums = add(k, ref[first:last, left:right], sums)
                else:
                    sums = lax.fori_loop(
                        0,
                        sources,
                        lambda a, sums: add(a, legendre_refs[0][a, first:last, left:right], sums),
                        (jnp.zeros((last - first, right - left), F32),) * count,
                    )
                for i in range(*own):
                    sums_ref[i, first:last, left:right] = sums[i - own[0]]
        for i in range(*own):
            value = sums_ref[i]
            folded = value[:, :slots]
            for lat in range(1, lats):
                folded = folded + value[:, lat * slots : (lat + 1) * slots]
            done_ref[i] = (folded * alive).T
            copies.append(pltpu.make_async_copy(done_ref.at[i], out_ref.at[i], sems.at[i]))
            copies[-1].start()
    for copy in copies:
        copy.wait()


def local(n_lat, n_wave, spectra, legendre, wave_m, nlon, coriolis, gauss_quadrature_weight):
    lats, slots, total = legendre.shape
    fields, levels = spectra.shape[:2]
    waves = wave_m.shape[0]
    degrees = spectra.shape[4]
    columns = lats * slots
    owned = lats * levels // n_wave
    lat_rank = lax.axis_index("lat").reshape(1)
    wave_rank = lax.axis_index("wave").reshape(1)
    steps = -(-(NLON // 8 + 1) // BASE)
    places = steps * BASE

    rows = legendre.reshape(columns, total)
    apart = n_lat in (2, 4, 8)
    if apart:
        blocks = call(
            turn_kernel,
            (jax.ShapeDtypeStruct((degrees, columns), BF16),) * n_lat,
            [SMEM, VMEM],
            [pltpu.VMEM((total, columns), BF16)],
            out_specs=(VMEM,) * n_lat,
            bytes_accessed=4 * total * columns,
        )(lat_rank, rows)
        turned = {0: blocks[0]}
        for d in ORDER[n_lat]:
            turned[d] = lax.ppermute(blocks[d], "lat", [(i, i ^ d) for i in range(n_lat)])
    else:
        blocks = call(
            turn_all_kernel,
            jax.ShapeDtypeStruct((total, columns), BF16),
            [VMEM],
            bytes_accessed=4 * total * columns,
        )(rows)
        blocks = lax.all_to_all(blocks.reshape(n_lat, degrees, columns), "lat", 0, 0, tiled=True)
        turned = {0: blocks}

    all_ids = wave_m.reshape(1, waves)
    spectra_turned, alive = call(
        functools.partial(turn_spectra_kernel, lats, fields),
        (
            jax.ShapeDtypeStruct((2 * fields * levels, degrees, columns), F32),
            jax.ShapeDtypeStruct((degrees, slots), F32),
        ),
        [SMEM, SMEM, VMEM, VMEM],
        out_specs=(VMEM, VMEM),
        flops=WORK * 10 * fields * levels * degrees * columns,
        bytes_accessed=8 * fields * levels * degrees * columns,
    )(lat_rank, wave_rank, spectra.reshape(2 * fields * levels, slots, degrees), all_ids)

    row = call(
        functools.partial(table_kernel, levels),
        (
            jax.ShapeDtypeStruct((owned, places, 2 * waves), BF16),
            jax.ShapeDtypeStruct((owned, 4, 8, waves), F32),
            jax.ShapeDtypeStruct((owned, 4, 8, waves), F32),
            jax.ShapeDtypeStruct((owned, 8, places), F32),
            jax.ShapeDtypeStruct((owned, 8, places), F32),
        ),
        [SMEM, VMEM, HBM, HBM, HBM],
        [
            pltpu.VMEM((2, BASE, waves), F32),
            pltpu.VMEM((2, steps, waves), F32),
            pltpu.SMEM((lats,), jnp.int32),
            pltpu.SMEM((lats,), F32),
            pltpu.SMEM((lats,), F32),
            pltpu.SemaphoreType.DMA((3,)),
        ],
        out_specs=(VMEM,) * 5,
        flops=WORK * 16 * owned * places * waves,
        bytes_accessed=4 * owned * places * waves,
    )(wave_rank, all_ids, *[far(x) for x in (nlon, coriolis, gauss_quadrature_weight)])
    spectra_turned, *row = lax.optimization_barrier((spectra_turned, *row))

    message = jax.ShapeDtypeStruct(
        (n_lat * n_wave, owned) + message_shape(2 * fields, slots), BF16
    )
    cost = WORK * 4 * fields * levels * degrees * columns
    if apart:
        groups = GROUPS[n_lat]
        early = []
        for part in groups[:-1]:
            early.append(
                call(
                    functools.partial(early_forward_kernel, levels, owned, slots),
                    jax.ShapeDtypeStruct((len(part) * n_wave,) + message.shape[1:], BF16),
                    [VMEM] * (1 + len(part)),
                    flops=len(part) * cost,
                    bytes_accessed=cost // WORK,
                )(spectra_turned, *[turned[d] for d in part])
            )
        partial = call(
            functools.partial(last_forward_kernel, levels, owned, slots, groups),
            message,
            [SMEM] + [VMEM] * (len(groups) + len(groups[-1])),
            flops=len(groups[-1]) * cost,
            bytes_accessed=cost // WORK,
        )(lat_rank, spectra_turned, *early, *[turned[d] for d in groups[-1]])
    else:
        partial = call(
            functools.partial(loop_forward_kernel, levels, owned, slots),
            message,
            [VMEM, VMEM],
            flops=n_lat * cost,
            bytes_accessed=cost // WORK,
        )(spectra_turned, turned[0])
    partial = lax.all_to_all(partial, ("lat", "wave"), 0, 0, tiled=True)

    back = call(
        functools.partial(grid_kernel, slots),
        jax.ShapeDtypeStruct((n_lat * n_wave, owned, 4, slots), BF16),
        [VMEM] * 6,
        [pltpu.VMEM((24, 2 * waves), F32)],
        flops=128 * owned * places * waves,
        bytes_accessed=4 * owned * places * waves,
    )(partial, *row)
    back = lax.all_to_all(back, ("lat", "wave"), 0, 0, tiled=True)

    outs = 4 * levels
    out = call(
        functools.partial(backward_kernel, levels),
        jax.ShapeDtypeStruct((outs, slots, degrees), F32),
        [SMEM, VMEM, VMEM] + [VMEM] * len(turned),
        [
            pltpu.VMEM((n_lat, outs, 8, columns), F32),
            pltpu.VMEM((outs, degrees, columns), F32),
            pltpu.VMEM((outs, slots, degrees), F32),
            pltpu.SemaphoreType.DMA((outs,)),
        ],
        out_specs=HBM,
        flops=2 * n_lat * outs * degrees * columns,
        bytes_accessed=8 * outs * degrees * slots,
    )(lat_rank, back, alive, *[turned[d] for d in sorted(turned)])
    return out.reshape(2, levels, 2, slots, degrees)


def solution(mesh):
    placed = (
        P(None, None, None, "wave", "lat"),
        P("lat", "wave", None),
        P(),
        P("lat"),
        P("lat"),
        P("lat"),
    )
    n_lat = mesh.shape["lat"]
    return jax.shard_map(
        functools.partial(local, n_lat, mesh.shape["wave"]),
        mesh=mesh,
        in_specs=placed,
        out_specs=P(None, None, None, "wave", "lat"),
        check_vma=False,
    )
```

```python
import functools
import math

import jax
import jax.numpy as jnp
from jax import lax
from jax.experimental import pallas as pl
from jax.experimental.pallas import tpu as pltpu
from jax.sharding import PartitionSpec as P

NLON = 3088
BASE = 16
LANES = 128
WORK = 128
ORDER = {2: (1,), 4: (2, 3, 1), 8: (6, 4, 7, 5, 3, 2, 1)}
GROUPS = {2: ((0,), (1,)), 4: ((0, 1), (2, 3)), 8: ((0, 1, 6), (4, 7), (2, 3), (5,))}

F32 = jnp.float32
BF16 = jnp.bfloat16

VMEM = pl.BlockSpec(memory_space=pltpu.VMEM)
SMEM = pl.BlockSpec(memory_space=pltpu.SMEM)
HBM = pl.BlockSpec(memory_space=pltpu.HBM)


def call(
    body, out_shape, in_specs, scratch=(), out_specs=VMEM, flops=0, bytes_accessed=0,
    grant=16 * 1024 * 1024,
):
    return pl.pallas_call(
        body,
        out_shape=out_shape,
        in_specs=in_specs,
        out_specs=out_specs,
        scratch_shapes=scratch,
        cost_estimate=pl.CostEstimate(
            flops=flops, bytes_accessed=bytes_accessed, transcendentals=0
        ),
        compiler_params=pltpu.CompilerParams(vmem_limit_bytes=grant),
    )


def far(value):
    return pltpu.with_memory_space_constraint(value, pltpu.HBM)


def pieces(extent, size):
    return [(first, min(first + size, extent)) for first in range(0, extent, size)]


def message_shape(rows, slots):
    if slots > LANES and slots % LANES == LANES // 2 and rows % 2 == 0:
        lines = rows * (slots // LANES) + rows // 2
        return (-(-lines // 2), 2, LANES)
    return (rows, slots)


def put_message(ref, index, value):
    if len(ref.shape) == len(index) + 2:
        ref[index] = value.astype(BF16)
        return
    rows, slots = value.shape
    lines = [value[:, first : first + LANES] for first in range(0, slots - LANES + 1, LANES)]
    rest = value[:, slots - LANES // 2 :]
    lines.append(jnp.concatenate([rest[: rows // 2], rest[rows // 2 :]], axis=1))
    if lines[-1].shape[0] % 2:
        lines.append(lines[-1][:1])
    lines = jnp.concatenate(lines, axis=0)
    for k in range(lines.shape[0] // 2):
        ref[index + (k,)] = lines[2 * k : 2 * k + 2].astype(BF16)


def get_message(message, rows, slots):
    if message.ndim == 2:
        return message
    lines = jnp.concatenate([message[k] for k in range(message.shape[0])], axis=0)
    whole = slots // LANES
    parts = [lines[k * rows : (k + 1) * rows] for k in range(whole)]
    rest = lines[whole * rows : whole * rows + rows // 2]
    half = LANES // 2
    parts.append(jnp.concatenate([rest[:, :half], rest[:, half:]], axis=0))
    return jnp.concatenate(parts, axis=1)


def segments(lats, slots):
    tail = slots - LANES // 2
    if lats == 2 and tail > 0 and tail % LANES == 0:
        own = [(lat, f, f + LANES) for f in range(0, tail, LANES) for lat in range(lats)]
        return own + [(lat, tail, slots) for lat in range(lats)]
    return [(lat, 0, slots) for lat in range(lats)]


def join(values, lats, slots):
    return jnp.concatenate([values[lat][:, f:l] for lat, f, l in segments(lats, slots)], axis=1)


def turn_kernel(lats, rank_ref, legendre_ref, *refs):
    *out_refs, turned_ref = refs
    slots = legendre_ref.shape[0] // lats
    for first, last in pieces(legendre_ref.shape[1], LANES):
        rows = [
            legendre_ref[lat * slots + f : lat * slots + l, first:last]
            for lat, f, l in segments(lats, slots)
        ]
        turned_ref[first:last, :] = jnp.concatenate(rows, axis=0).T
    degrees = turned_ref.shape[0] // len(out_refs)
    for d, out_ref in enumerate(out_refs):
        start = (rank_ref[0] ^ d) * degrees
        if degrees % 16 == 0:
            start = pl.multiple_of(start, 16)
        out_ref[...] = turned_ref[pl.ds(start, degrees), :]


def turn_all_kernel(lats, legendre_ref, out_ref):
    slots = legendre_ref.shape[0] // lats
    for first, last in pieces(legendre_ref.shape[1], LANES):
        rows = [
            legendre_ref[lat * slots + f : lat * slots + l, first:last]
            for lat, f, l in segments(lats, slots)
        ]
        out_ref[first:last, :] = jnp.concatenate(rows, axis=0).T


def turn_spectra_kernel(
    repeats, fields, lat_ref, wave_ref, spectra_ref, ids_ref, out_ref, alive_ref
):
    count, slots, degrees = spectra_ref.shape
    levels = count // (2 * fields)
    ids = jnp.zeros((1, slots), jnp.int32)
    for w, (first, last) in enumerate(pieces(ids_ref.shape[1], slots)):
        ids = jnp.where(wave_ref[0] == w, ids_ref[:, first:last], ids)
    degree = lat_ref[0] * degrees + lax.broadcasted_iota(jnp.int32, (degrees, slots), 0)
    alive_ref[...] = jnp.where(degree >= ids, 1.0, 0.0)
    alive = alive_ref[...]
    for i in range(count):
        field, level, part = i // (2 * levels), (i // 2) % levels, i % 2
        turned = spectra_ref[i].astype(F32).T * alive
        place = (level * fields + field) * 2 + part
        out_ref[place] = join([turned] * repeats, repeats, slots)


def forward_sums(legendre_refs, spectra_ref):
    degrees, columns = legendre_refs[0].shape
    fields = spectra_ref.shape[0]
    tiles = [[] for _ in legendre_refs]
    for left, right in pieces(columns, LANES):
        sums = [[None] * fields for _ in legendre_refs]
        for first, last in pieces(degrees, 16):
            own = [ref[first:last, left:right].astype(F32) for ref in legendre_refs]
            for i in range(fields):
                other = spectra_ref[i, first:last, left:right]
                for k, value in enumerate(own):
                    product = value * other
                    if last - first == 16:
                        product = product[:8] + product[8:]
                    else:
                        product = jnp.sum(product, axis=0, keepdims=True)
                    sums[k][i] = product if sums[k][i] is None else sums[k][i] + product
        for tile, values in zip(tiles, sums):
            rows = [jnp.sum(value, axis=0, keepdims=True) for value in values]
            tile.append(jnp.concatenate(rows, axis=0))
    return [jnp.concatenate(tile, axis=1) for tile in tiles]


def put_row_messages(levels, owned, slots, out_ref, a, value):
    per_level = value.shape[0] // levels
    rows = value.shape[1] // slots * levels
    lats = rows // levels
    for row in range(rows):
        lat, level = row // levels, row % levels
        own = value[level * per_level : (level + 1) * per_level]
        stretches = []
        column = 0
        for other, first, last in segments(lats, slots):
            if other == lat:
                stretches.append(own[:, column : column + last - first])
            column += last - first
        message = jnp.concatenate(stretches, axis=1)
        put_message(out_ref, (a * (rows // owned) + row // owned, row % owned), message)


def early_forward_kernel(levels, owned, slots, spectra_ref, *refs):
    *legendre_refs, out_ref = refs
    for first, last in pieces(len(legendre_refs), 2):
        for k, value in enumerate(forward_sums(legendre_refs[first:last], spectra_ref)):
            put_row_messages(levels, owned, slots, out_ref, first + k, value)


def last_forward_kernel(levels, owned, slots, groups, rank_ref, spectra_ref, *refs):
    *early_refs, out_ref = refs[: len(groups) - 1] + refs[-1:]
    legendre_refs = refs[len(groups) - 1 : -1]
    for places, ref in zip(groups[:-1], early_refs):
        targets = ref.shape[0] // len(places)
        for k, d in enumerate(places):
            start = (rank_ref[0] ^ d) * targets
            out_ref[pl.ds(start, targets)] = ref[k * targets : (k + 1) * targets]
    for first, last in pieces(len(legendre_refs), 2):
        values = forward_sums(legendre_refs[first:last], spectra_ref)
        for d, value in zip(groups[-1][first:last], values):
            put_row_messages(levels, owned, slots, out_ref, rank_ref[0] ^ d, value)


def loop_forward_kernel(levels, owned, slots, spectra_ref, legendre_ref, out_ref):
    def one_source(a, carry):
        (value,) = forward_sums([legendre_ref.at[a]], spectra_ref)
        put_row_messages(levels, owned, slots, out_ref, a, value)
        return carry

    lax.fori_loop(0, legendre_ref.shape[0], one_source, 0)


def cos_sin(places, ids, count, inverse):
    quads = 4.0 * places * ids
    turns = jnp.floor(quads * inverse + 0.5)
    angle = (quads - turns * count) * (inverse * (math.pi / 2))
    square = angle * angle
    c = 1.0 + square * (-1 / 2 + square * (1 / 24 + square * (-1 / 720 + square * (1 / 40320))))
    s = angle * (
        1.0 + square * (-1 / 6 + square * (1 / 120 + square * (-1 / 5040 + square * (1 / 362880))))
    )
    quadrant = turns - 4.0 * jnp.floor(turns * 0.25)
    odd = (quadrant == 1.0) | (quadrant == 3.0)
    cosine = jnp.where(odd, s, c)
    sine = jnp.where(odd, c, s)
    cosine = jnp.where((quadrant == 1.0) | (quadrant == 2.0), -cosine, cosine)
    sine = jnp.where(quadrant >= 2.0, -sine, sine)
    return cosine, sine


def image_signs(ids):
    quadrant = ids - 4.0 * jnp.floor(ids * 0.25)
    one = jnp.ones_like(ids)
    none = jnp.zeros_like(ids)
    parity = jnp.where((quadrant == 1.0) | (quadrant == 3.0), -1.0, 1.0)
    c = jnp.where(quadrant == 0.0, 1.0, jnp.where(quadrant == 2.0, -1.0, 0.0))
    s = jnp.where(quadrant == 1.0, 1.0, jnp.where(quadrant == 3.0, -1.0, 0.0))
    cos_cos = [one, one, parity, parity, c, c, c, c]
    cos_sin = [none, none, none, none, s, -s, -s, s]
    sin_cos = [none, none, none, none, s, s, -s, -s]
    sin_sin = [one, -one, -parity, parity, -c, c, -c, c]
    return [jnp.concatenate(rows, axis=0) for rows in (cos_cos, cos_sin, sin_cos, sin_sin)]


def table_kernel(
    levels, rank_ref, ids_ref, nlon_far, coriolis_far, weight_far,
    table_ref, left_ref, right_ref, share_ref, rotation_ref,
    base_ref, step_ref, nlon_ref, coriolis_ref, weight_ref, sems,
):
    copies = [
        pltpu.make_async_copy(far, near, sems.at[i])
        for i, (far, near) in enumerate(
            [(nlon_far, nlon_ref), (coriolis_far, coriolis_ref), (weight_far, weight_ref)]
        )
    ]
    for copy in copies:
        copy.start()
    for copy in copies:
        copy.wait()
    owned = table_ref.shape[0]
    steps = step_ref.shape[1]
    waves = ids_ref.shape[1]
    ids = ids_ref[...].astype(F32)
    signs = image_signs(ids)
    for offset in range(owned):
        latitude = (rank_ref[0] * owned + offset) // levels
        count_int = nlon_ref[latitude]
        count = jnp.full((1, waves), count_int.astype(F32))
        inverse = 1.0 / count
        rows = lax.broadcasted_iota(jnp.int32, (BASE, waves), 0).astype(F32)
        base_ref[0], base_ref[1] = cos_sin(rows, ids, count, inverse)
        rows = lax.broadcasted_iota(jnp.int32, (steps, waves), 0).astype(F32) * BASE
        step_ref[0], step_ref[1] = cos_sin(rows, ids, count, inverse)
        for a in range(steps):
            step_c = step_ref[0, a : a + 1, :]
            step_s = step_ref[1, a : a + 1, :]
            base_c = base_ref[0]
            base_s = base_ref[1]
            here = slice(a * BASE, (a + 1) * BASE)
            table_ref[offset, here, :waves] = (step_c * base_c - step_s * base_s).astype(BF16)
            table_ref[offset, here, waves:] = (step_s * base_c + step_c * base_s).astype(BF16)

        factor = jnp.where(ids == 0.0, 1.0, 2.0)
        factor = jnp.where(2.0 * ids < count, factor, 0.0)
        scale = jnp.where(factor > 0.0, weight_ref[latitude] / count, 0.0)
        left_ref[offset, 0] = signs[0] * factor
        left_ref[offset, 1] = -signs[2] * factor
        left_ref[offset, 2] = signs[1] * factor
        left_ref[offset, 3] = -signs[3] * factor
        right_ref[offset, 0] = signs[0] * scale
        right_ref[offset, 1] = signs[1] * scale
        right_ref[offset, 2] = -signs[2] * scale
        right_ref[offset, 3] = -signs[3] * scale
        place = lax.broadcasted_iota(jnp.int32, share_ref.shape[1:], 1)
        share = jnp.where((place == 0) | (8 * place == count_int), 0.5, 1.0)
        share_ref[offset] = jnp.where(8 * place <= count_int, share, 0.0)
        rotation_ref[offset] = jnp.full(rotation_ref.shape[1:], coriolis_ref[latitude])


def grid_kernel(
    slots, partial_ref, table_ref, left_ref, right_ref, share_ref, rotation_ref, out_ref, rows_ref
):
    owned = partial_ref.shape[1]
    waves = left_ref.shape[-1]
    parts = waves // slots
    sources = partial_ref.shape[0] // parts
    for offset in range(owned):

        def total(w):
            def add(a, value):
                return value + partial_ref[a * parts + w, offset].astype(F32)

            if sources > 8:
                return lax.fori_loop(1, sources, add, partial_ref[w, offset].astype(F32))
            value = partial_ref[w, offset].astype(F32)
            for a in range(1, sources):
                value = add(a, value)
            return value

        fourier = jnp.concatenate(
            [get_message(total(w), 6, slots) for w in range(parts)], axis=1
        )
        fourier = fourier.astype(BF16).astype(F32)
        for field in range(3):
            here = slice(8 * field, 8 * field + 8)
            real = fourier[2 * field : 2 * field + 1]
            imag = fourier[2 * field + 1 : 2 * field + 2]
            rows_ref[here, :waves] = real * left_ref[offset, 0] + imag * left_ref[offset, 1]
            rows_ref[here, waves:] = real * left_ref[offset, 2] + imag * left_ref[offset, 3]
        grid = lax.dot_general(
            rows_ref[...].astype(BF16),
            table_ref[offset],
            (((1,), (1,)), ((), ())),
            preferred_element_type=F32,
        )
        vorticity, divergence, temperature = grid[0:8], grid[8:16], grid[16:24]
        share = share_ref[offset]

        def shared(product):
            rounded = jnp.where(share > 0.0, product, 0.0).astype(BF16)
            return rounded.astype(F32) * share

        stretch = shared(-(vorticity + rotation_ref[offset]) * divergence)
        heating = shared(-temperature * divergence)
        products = jnp.concatenate([stretch, heating], axis=0).astype(BF16)
        sums = jnp.dot(products, table_ref[offset], preferred_element_type=F32)
        both = []
        for q in range(2):
            c = sums[8 * q : 8 * q + 8, :waves]
            s = sums[8 * q : 8 * q + 8, waves:]
            for k in range(2):
                term = c * right_ref[offset, 2 * k] + s * right_ref[offset, 2 * k + 1]
                both.append(jnp.sum(term, axis=0, keepdims=True))
        back = jnp.concatenate(both, axis=0)
        for w in range(parts):
            part = back[:, w * slots : (w + 1) * slots]

            def put(a, carry):
                put_message(out_ref, (a * parts + w, offset), part)
                return carry

            if sources > 8:
                lax.fori_loop(0, sources, put, 0)
            else:
                for a in range(sources):
                    put(a, 0)


def backward_kernel(levels, rank_ref, back_ref, alive_ref, *refs):
    *legendre_refs, out_ref, wide_ref, sums_ref, done_ref, sems = refs
    sources, _, _, columns = wide_ref.shape
    degrees = sums_ref.shape[1]
    outs, slots, _ = out_ref.shape
    lats = columns // slots
    owned = back_ref.shape[1]
    targets = back_ref.shape[0] // sources
    apart = len(legendre_refs) > 1

    def spread(k, a):
        for level in range(levels):
            rows = []
            for lat in range(lats):
                row = lat * levels + level
                rows.append(back_ref[a * targets + row // owned, row % owned].astype(F32))
            both = join(rows, lats, slots)
            for i in range(4):
                place = ((i // 2) * levels + level) * 2 + i % 2
                wide_ref[k, place] = jnp.broadcast_to(both[i : i + 1], (8, columns))

    if apart:
        for d in range(sources):
            spread(d, rank_ref[0] ^ d)
    else:
        lax.fori_loop(0, sources, lambda a, carry: spread(a, a) or carry, 0)

    alive = alive_ref[...]
    order = segments(lats, slots)
    folds = len(order) > lats
    if folds:
        sets = [
            ([(lats * f, lats * f + LANES), (lats * f + LANES, lats * f + 2 * LANES)], f, LANES)
            for f in range(0, slots - LANES // 2, LANES)
        ]
        sets.append(([(columns - LANES, columns)], slots - LANES // 2, LANES // 2))
    else:
        sets = [([(left, right)], left, right - left) for left, right in pieces(columns, LANES)]
    for first, last in pieces(degrees, 16):
        for tiles, begin, width in sets:
            extent = tiles[0][1] - tiles[0][0]

            def add(k, piece_of, sums):
                sums = list(sums)
                for left, right in tiles:
                    piece = piece_of(left, right).astype(F32)
                    for i in range(outs):
                        other = wide_ref[k, i, :, left:right]
                        other = jnp.concatenate([other, other], axis=0)[: last - first]
                        term = piece * other
                        sums[i] = term if sums[i] is None else sums[i] + term
                return tuple(sums)

            if apart:
                sums = (None,) * outs
                for k, ref in enumerate(legendre_refs):
                    sums = add(k, lambda l, r, ref=ref: ref[first:last, l:r], sums)
            else:
                sums = lax.fori_loop(
                    0,
                    sources,
                    lambda a, sums: add(a, lambda l, r: legendre_refs[0][a, first:last, l:r], sums),
                    (jnp.zeros((last - first, extent), F32),) * outs,
                )
            for i in range(outs):
                value = sums[i]
                if width < extent:
                    value = value[:, :width] + value[:, width:]
                sums_ref[i, first:last, begin : begin + width] = value
    copies = []
    for i in range(outs):
        value = sums_ref[i]
        folded = value[:, :slots]
        if not folds:
            for lat in range(1, lats):
                folded = folded + value[:, lat * slots : (lat + 1) * slots]
        done_ref[i] = (folded * alive).T
        copies.append(pltpu.make_async_copy(done_ref.at[i], out_ref.at[i], sems.at[i]))
        copies[-1].start()
    for copy in copies:
        copy.wait()


def local(n_lat, n_wave, spectra, legendre, wave_m, nlon, coriolis, gauss_quadrature_weight):
    lats, slots, total = legendre.shape
    fields, levels = spectra.shape[:2]
    waves = wave_m.shape[0]
    degrees = spectra.shape[4]
    columns = lats * slots
    owned = lats * levels // n_wave
    lat_rank = lax.axis_index("lat").reshape(1)
    wave_rank = lax.axis_index("wave").reshape(1)
    steps = -(-(NLON // 8 + 1) // BASE)
    places = steps * BASE

    rows = legendre.reshape(columns, total)
    apart = n_lat in (2, 4, 8)
    if apart:
        blocks = call(
            functools.partial(turn_kernel, lats),
            (jax.ShapeDtypeStruct((degrees, columns), BF16),) * n_lat,
            [SMEM, VMEM],
            [pltpu.VMEM((total, columns), BF16)],
            out_specs=(VMEM,) * n_lat,
            bytes_accessed=4 * total * columns,
        )(lat_rank, rows)
        turned = {0: blocks[0]}
        for d in ORDER[n_lat]:
            turned[d] = lax.ppermute(blocks[d], "lat", [(i, i ^ d) for i in range(n_lat)])
    else:
        blocks = call(
            functools.partial(turn_all_kernel, lats),
            jax.ShapeDtypeStruct((total, columns), BF16),
            [VMEM],
            bytes_accessed=4 * total * columns,
        )(rows)
        blocks = lax.all_to_all(blocks.reshape(n_lat, degrees, columns), "lat", 0, 0, tiled=True)
        turned = {0: blocks}

    all_ids = wave_m.reshape(1, waves)
    spectra_turned, alive = call(
        functools.partial(turn_spectra_kernel, lats, fields),
        (
            jax.ShapeDtypeStruct((2 * fields * levels, degrees, columns), F32),
            jax.ShapeDtypeStruct((degrees, slots), F32),
        ),
        [SMEM, SMEM, VMEM, VMEM],
        out_specs=(VMEM, VMEM),
        flops=WORK * 10 * fields * levels * degrees * columns,
        bytes_accessed=8 * fields * levels * degrees * columns,
    )(lat_rank, wave_rank, spectra.reshape(2 * fields * levels, slots, degrees), all_ids)

    row = call(
        functools.partial(table_kernel, levels),
        (
            jax.ShapeDtypeStruct((owned, places, 2 * waves), BF16),
            jax.ShapeDtypeStruct((owned, 4, 8, waves), F32),
            jax.ShapeDtypeStruct((owned, 4, 8, waves), F32),
            jax.ShapeDtypeStruct((owned, 8, places), F32),
            jax.ShapeDtypeStruct((owned, 8, places), F32),
        ),
        [SMEM, VMEM, HBM, HBM, HBM],
        [
            pltpu.VMEM((2, BASE, waves), F32),
            pltpu.VMEM((2, steps, waves), F32),
            pltpu.SMEM((lats,), jnp.int32),
            pltpu.SMEM((lats,), F32),
            pltpu.SMEM((lats,), F32),
            pltpu.SemaphoreType.DMA((3,)),
        ],
        out_specs=(VMEM,) * 5,
        flops=WORK * 16 * owned * places * waves,
        bytes_accessed=4 * owned * places * waves,
    )(wave_rank, all_ids, *[far(x) for x in (nlon, coriolis, gauss_quadrature_weight)])
    spectra_turned, *row = lax.optimization_barrier((spectra_turned, *row))

    message = jax.ShapeDtypeStruct(
        (n_lat * n_wave, owned) + message_shape(2 * fields, slots), BF16
    )
    cost = WORK * 4 * fields * levels * degrees * columns
    if apart:
        groups = GROUPS[n_lat]
        early = []
        for part in groups[:-1]:
            early.append(
                call(
                    functools.partial(early_forward_kernel, levels, owned, slots),
                    jax.ShapeDtypeStruct((len(part) * n_wave,) + message.shape[1:], BF16),
                    [VMEM] * (1 + len(part)),
                    flops=len(part) * cost,
                    bytes_accessed=cost // WORK,
                )(spectra_turned, *[turned[d] for d in part])
            )
        partial = call(
            functools.partial(last_forward_kernel, levels, owned, slots, groups),
            message,
            [SMEM] + [VMEM] * (len(groups) + len(groups[-1])),
            flops=len(groups[-1]) * cost,
            bytes_accessed=cost // WORK,
        )(lat_rank, spectra_turned, *early, *[turned[d] for d in groups[-1]])
    else:
        partial = call(
            functools.partial(loop_forward_kernel, levels, owned, slots),
            message,
            [VMEM, VMEM],
            flops=n_lat * cost,
            bytes_accessed=cost // WORK,
        )(spectra_turned, turned[0])
    partial = lax.all_to_all(partial, ("lat", "wave"), 0, 0, tiled=True)

    back = call(
        functools.partial(grid_kernel, slots),
        jax.ShapeDtypeStruct((n_lat * n_wave, owned, 4, slots), BF16),
        [VMEM] * 6,
        [pltpu.VMEM((24, 2 * waves), F32)],
        flops=128 * owned * places * waves,
        bytes_accessed=4 * owned * places * waves,
    )(partial, *row)
    back = lax.all_to_all(back, ("lat", "wave"), 0, 0, tiled=True)

    outs = 4 * levels
    out = call(
        functools.partial(backward_kernel, levels),
        jax.ShapeDtypeStruct((outs, slots, degrees), F32),
        [SMEM, VMEM, VMEM] + [VMEM] * len(turned),
        [
            pltpu.VMEM((n_lat, outs, 8, columns), F32),
            pltpu.VMEM((outs, degrees, columns), F32),
            pltpu.VMEM((outs, slots, degrees), F32),
            pltpu.SemaphoreType.DMA((outs,)),
        ],
        out_specs=HBM,
        flops=2 * n_lat * outs * degrees * columns,
        bytes_accessed=8 * outs * degrees * slots,
    )(lat_rank, back, alive, *[turned[d] for d in sorted(turned)])
    return out.reshape(2, levels, 2, slots, degrees)


def solution(mesh):
    placed = (
        P(None, None, None, "wave", "lat"),
        P("lat", "wave", None),
        P(),
        P("lat"),
        P("lat"),
        P("lat"),
    )
    n_lat = mesh.shape["lat"]
    return jax.shard_map(
        functools.partial(local, n_lat, mesh.shape["wave"]),
        mesh=mesh,
        in_specs=placed,
        out_specs=P(None, None, None, "wave", "lat"),
        check_vma=False,
    )
```
